8 devices in a mesh: prompts: 1 (over z), model: 2 (over y), resp: 4 (over x, core).
Axes of the slice: x: 2, y: 2, z: 1, core: 2. Of those that a mesh axis runs over, the one named last changes fastest.
Arguments:
- x_prompt: bfloat16 [256, 896], P(('prompts', 'resp'))
- x_resp: bfloat16 [4, 256, 896], P(('prompts', 'resp'))
- targets: int32 [4, 256], P(('prompts', 'resp'))
- attn_norm: float32 [2, 896], replicated
- mlp_norm: float32 [2, 896], replicated
- w_q: bfloat16 [2, 896, 14, 64], P(None, None, 'model')
- w_k: bfloat16 [2, 896, 2, 64], P(None, None, 'model')
- w_v: bfloat16 [2, 896, 2, 64], P(None, None, 'model')
- w_o: bfloat16 [2, 14, 64, 896], P(None, 'model')
- w_gate: bfloat16 [2, 896, 4864], P(None, None, 'model')
- w_up: bfloat16 [2, 896, 4864], P(None, None, 'model')
- w_down: bfloat16 [2, 4864, 896], P(None, 'model')
- final_norm: float32 [896], replicated
- w_head: bfloat16 [896, 4096], P(None, 'model')
Outputs:
- output: float32 [4, 256], P(('prompts', 'resp'))
All inputs are finite; a program needn't handle non-finite values.
Results may differ from the reference program's by a relative error of at most 0.00312084.
Values are sent between devices in bfloat16 or wider.
A program may use at most 1 GiB of HBM per device.

```python
import math
import jax
import jax.numpy as jnp
from jax import lax

D_MODEL = 896
N_HEADS = 14
KV_HEADS = 2
HEAD_DIM = 64
FF_DIM = 4864
PROMPT_DEV = 64
RESP_LEN = 256
VOCAB_SLICE = 4096
GROUP_SIZE = 4
N_LAYERS = 2
ROPE_BASE = 10000
PROMPT_LEN = PROMPT_DEV * GROUP_SIZE
Q_GROUP = N_HEADS // KV_HEADS
RMS_EPS = 1e-6
NEG_BIG = -1e30


def setup_inputs(seed: int = 0, part: int = 0) -> dict:
    root_key = jax.random.key(seed)
    data_root, weight_root = jax.random.split(root_key)
    data_keys = jax.random.split(jax.random.fold_in(data_root, part), 5)
    weight_keys = jax.random.split(weight_root, 12)

    def normal_weight(rng_key, arr_shape, fan_in, w_gain):
        raw_draw = jax.random.normal(rng_key, arr_shape, jnp.float32)
        return (raw_draw * (w_gain / math.sqrt(fan_in))).astype(jnp.bfloat16)

    def norm_gains(rng_key, arr_shape):
        return jax.random.uniform(rng_key, arr_shape, jnp.float32, 0.5, 1.5)

    prompt_mean = jax.random.normal(data_keys[0], (1, D_MODEL), jnp.float32) * 0.7
    piece_shift = jax.random.normal(data_keys[1], (GROUP_SIZE, 1, D_MODEL), jnp.float32) * 0.7
    prompt_noise = jax.random.normal(data_keys[2], (GROUP_SIZE, PROMPT_DEV, D_MODEL), jnp.float32)
    x_prompt = (prompt_noise + piece_shift + prompt_mean).reshape(PROMPT_LEN, D_MODEL).astype(jnp.bfloat16)
    x_resp = jax.random.normal(data_keys[3], (GROUP_SIZE, RESP_LEN, D_MODEL), jnp.float32).astype(jnp.bfloat16)
    flat_ids = jax.random.randint(data_keys[4], (GROUP_SIZE * RESP_LEN,), 0, VOCAB_SLICE, dtype=jnp.int32)
    slot_ids = jnp.arange(GROUP_SIZE * RESP_LEN)
    flat_ids = jnp.where(slot_ids == 0, VOCAB_SLICE - 1, jnp.where(slot_ids == 1, 0, flat_ids))
    targets = flat_ids.reshape(GROUP_SIZE, RESP_LEN).astype(jnp.int32)
    return {
        'x_prompt': x_prompt,
        'x_resp': x_resp,
        'targets': targets,
        'attn_norm': norm_gains(weight_keys[0], (N_LAYERS, D_MODEL)),
        'mlp_norm': norm_gains(weight_keys[1], (N_LAYERS, D_MODEL)),
        'w_q': normal_weight(weight_keys[2], (N_LAYERS, D_MODEL, N_HEADS, HEAD_DIM), D_MODEL, 1.0),
        'w_k': normal_weight(weight_keys[3], (N_LAYERS, D_MODEL, KV_HEADS, HEAD_DIM), D_MODEL, 1.0),
        'w_v': normal_weight(weight_keys[4], (N_LAYERS, D_MODEL, KV_HEADS, HEAD_DIM), D_MODEL, 1.0),
        'w_o': normal_weight(weight_keys[5], (N_LAYERS, N_HEADS, HEAD_DIM, D_MODEL), N_HEADS * HEAD_DIM, 1.0),
        'w_gate': normal_weight(weight_keys[6], (N_LAYERS, D_MODEL, FF_DIM), D_MODEL, 1.0),
        'w_up': normal_weight(weight_keys[7], (N_LAYERS, D_MODEL, FF_DIM), D_MODEL, 1.0),
        'w_down': normal_weight(weight_keys[8], (N_LAYERS, FF_DIM, D_MODEL), FF_DIM, 1.0),
        'final_norm': norm_gains(weight_keys[9], (D_MODEL,)),
        'w_head': normal_weight(weight_keys[10], (D_MODEL, VOCAB_SLICE), D_MODEL, 3.0),
    }


def rms_norm(x_in, norm_gain):
    x_f = x_in.astype(jnp.float32)
    mean_sq = jnp.mean(x_f * x_f, axis=-1, keepdims=True)
    return (x_f * lax.rsqrt(mean_sq + RMS_EPS) * norm_gain).astype(jnp.bfloat16)


def rope_tables(positions):
    inv_freq = jnp.exp(jnp.arange(0, HEAD_DIM, 2, dtype=jnp.float32) * (-math.log(ROPE_BASE) / HEAD_DIM))
    angles = positions.astype(jnp.float32)[:, None] * inv_freq[None, :]
    return jnp.cos(angles), jnp.sin(angles)


def apply_rope(proj_f, cos_tab, sin_tab):
    half_dim = proj_f.shape[-1] // 2
    lo_half = proj_f[..., :half_dim]
    hi_half = proj_f[..., half_dim:]
    cos_b = cos_tab[:, None, :]
    sin_b = sin_tab[:, None, :]
    return jnp.concatenate([lo_half * cos_b - hi_half * sin_b, hi_half * cos_b + lo_half * sin_b], axis=-1)


def project_heads(hidden, w_mat):
    n_out = w_mat.shape[1] * w_mat.shape[2]
    proj_flat = jnp.dot(hidden, w_mat.reshape(D_MODEL, n_out), preferred_element_type=jnp.float32)
    return proj_flat.reshape(hidden.shape[0], w_mat.shape[1], HEAD_DIM)


def attend(queries, key_rows, val_rows, q_pos, k_pos):
    q_len = queries.shape[0]
    q_grp = queries.reshape(q_len, KV_HEADS, Q_GROUP, HEAD_DIM).astype(jnp.float32)
    scores = jnp.einsum('qhre,khe->hrqk', q_grp, key_rows.astype(jnp.float32)) * (1.0 / math.sqrt(HEAD_DIM))
    scores = jnp.where(k_pos[None, :] <= q_pos[:, None], scores, NEG_BIG)
    attn_probs = jax.nn.softmax(scores, axis=-1).astype(jnp.bfloat16).astype(jnp.float32)
    attn_mix = jnp.einsum('hrqk,khe->qhre', attn_probs, val_rows.astype(jnp.float32))
    return attn_mix.reshape(q_len, N_HEADS, HEAD_DIM).astype(jnp.bfloat16)


def finish_layer(x_in, attn_mix, w_out, gain_mlp, w_gate_l, w_up_l, w_down_l):
    attn_proj = jnp.dot(attn_mix.reshape(attn_mix.shape[0], N_HEADS * HEAD_DIM), w_out.reshape(N_HEADS * HEAD_DIM, D_MODEL), preferred_element_type=jnp.float32)
    x_mid = (x_in.astype(jnp.float32) + attn_proj).astype(jnp.bfloat16)
    hidden = rms_norm(x_mid, gain_mlp)
    gate_proj = jnp.dot(hidden, w_gate_l, preferred_element_type=jnp.float32)
    up_proj = jnp.dot(hidden, w_up_l, preferred_element_type=jnp.float32)
    act_vals = (jax.nn.silu(gate_proj) * up_proj).astype(jnp.bfloat16)
    down_proj = jnp.dot(act_vals, w_down_l, preferred_element_type=jnp.float32)
    return (x_mid.astype(jnp.float32) + down_proj).astype(jnp.bfloat16)


def reference(x_prompt, x_resp, targets, attn_norm, mlp_norm, w_q, w_k, w_v, w_o, w_gate, w_up, w_down, final_norm, w_head):
    prompt_pos = jnp.arange(PROMPT_LEN)
    resp_pos = PROMPT_LEN + jnp.arange(RESP_LEN)
    all_pos = jnp.concatenate([prompt_pos, resp_pos])
    p_cos, p_sin = rope_tables(prompt_pos)
    r_cos, r_sin = rope_tables(resp_pos)

    def kv_of(hidden, layer_idx, cos_tab, sin_tab):
        k_rot = apply_rope(project_heads(hidden, w_k[layer_idx]), cos_tab, sin_tab).astype(jnp.bfloat16)
        v_proj = project_heads(hidden, w_v[layer_idx]).astype(jnp.bfloat16)
        return k_rot, v_proj

    hidden_p = rms_norm(x_prompt, attn_norm[0])
    q_prompt = apply_rope(project_heads(hidden_p, w_q[0]), p_cos, p_sin).astype(jnp.bfloat16)
    k_one, v_one = kv_of(hidden_p, 0, p_cos, p_sin)

    def prompt_block(block_in):
        q_block, pos_block = block_in
        return attend(q_block, k_one, v_one, pos_block, prompt_pos)

    mix_prompt = lax.map(prompt_block, (q_prompt.reshape(GROUP_SIZE, PROMPT_DEV, N_HEADS, HEAD_DIM), prompt_pos.reshape(GROUP_SIZE, PROMPT_DEV)))
    x_prompt_one = finish_layer(x_prompt, mix_prompt.reshape(PROMPT_LEN, N_HEADS, HEAD_DIM), w_o[0], mlp_norm[0], w_gate[0], w_up[0], w_down[0])
    k_two, v_two = kv_of(rms_norm(x_prompt_one, attn_norm[1]), 1, p_cos, p_sin)
    prompt_cache = ((k_one, v_one), (k_two, v_two))

    def one_response(resp_in):
        x_cur, tgt_row = resp_in
        for layer_idx in range(N_LAYERS):
            k_cache, v_cache = prompt_cache[layer_idx]
            hidden = rms_norm(x_cur, attn_norm[layer_idx])
            q_resp = apply_rope(project_heads(hidden, w_q[layer_idx]), r_cos, r_sin).astype(jnp.bfloat16)
            k_resp, v_resp = kv_of(hidden, layer_idx, r_cos, r_sin)
            attn_mix = attend(q_resp, jnp.concatenate([k_cache, k_resp]), jnp.concatenate([v_cache, v_resp]), resp_pos, all_pos)
            x_cur = finish_layer(x_cur, attn_mix, w_o[layer_idx], mlp_norm[layer_idx], w_gate[layer_idx], w_up[layer_idx], w_down[layer_idx])
        logits = jnp.dot(rms_norm(x_cur, final_norm), w_head, preferred_element_type=jnp.float32)
        log_norm = jax.nn.logsumexp(logits, axis=-1)
        picked = jnp.sum(jnp.where(jnp.arange(VOCAB_SLICE)[None, :] == tgt_row[:, None], logits, 0.0), axis=-1)
        return picked - log_norm

    return lax.map(one_response, (x_resp, targets))
```

```python
import functools
import math

import jax
import jax.numpy as jnp
import numpy as np
from jax import lax
from jax.experimental import pallas as pl
from jax.experimental.pallas import tpu as pltpu
from jax.sharding import PartitionSpec as P

RMS_EPS = 1e-6
ROPE_BASE = 10000.0
NEG_BIG = -1e30
BF16 = jnp.bfloat16
F32 = jnp.float32

D = 896
HD = 64
PIECE = 64
RESP = 256
PROMPT = 256
ROWS = PIECE + RESP
FF = 2432
VOC = 2048
QROWS = 448
GROUP = 4
GAIN_PAD = 1024
CHUNKS = ((0, 64), (64, 128), (192, 128))
WO_QUARTER = QROWS // GROUP
WO_PIECES = ((0, 64), (64, 48))
FF_BLOCKS = ((0, 512), (512, 512), (1024, 512), (1536, 512), (2048, 384))


def rope_constants():
    inv = np.exp(np.arange(0, HD, 2, dtype=np.float32) * np.float32(-math.log(ROPE_BASE) / HD)).astype(np.float32)
    ang = np.arange(PROMPT + RESP, dtype=np.float32)[:, None] * inv[None, :]
    cos, sin = np.cos(ang).astype(np.float32), np.sin(ang).astype(np.float32)
    return np.concatenate([cos] * 4, axis=1), np.concatenate([-sin, sin] * 2, axis=1)


def mm(a, b):
    return jnp.dot(a, b, preferred_element_type=F32)


def mm_t(a, b):
    return lax.dot_general(a, b, (((1,), (1,)), ((), ())), preferred_element_type=F32)


def rms(x_f, gain):
    mean_sq = jnp.mean(x_f * x_f, axis=-1, keepdims=True)
    return (x_f * lax.rsqrt(mean_sq + RMS_EPS) * gain).astype(BF16)


def kernel(xp, xr, tgt, an, mn, wq, wk, wv, wo, wg, wu, wd, fn, wh, cs, sn, out,
           vx, vcs, vsn, vtgt, van, vmn, vfn, wqkv, womy, woot, vg, vu, vd, vh,
           kv, qb, amine, asnd, arcv, xm, ub, part, prcv, x1, hb, lgt, st_s, st_r,
           lsem, ssem, rsem):
    me = lax.axis_index('resp')
    side = lax.axis_index('model')
    other = 1 - side
    y_peer = {'model': other}
    d_peer = {'resp': me + 1 - 2 * lax.rem(me, 2)}
    x_peer = {'resp': lax.rem(me + 2, 4)}

    counts = {'l': 0, 'r': 0}

    def load(src, dst):
        cp = pltpu.make_async_copy(src, dst, lsem.at[counts['l']])
        counts['l'] += 1
        cp.start()
        return cp

    def remote(src, dst, peer):
        k = counts['r']
        counts['r'] += 1
        return pltpu.make_async_remote_copy(src_ref=src, dst_ref=dst, send_sem=ssem.at[k], recv_sem=rsem.at[k],
                                            device_id=peer, device_id_type=pl.DeviceIdType.MESH)

    sent = []

    def send(cp):
        cp.start()
        sent.append(cp)
        return cp

    def load_qkv(l):
        return [load(wq.at[l], wqkv.at[l, pl.ds(0, QROWS)]), load(wk.at[l], wqkv.at[l, pl.ds(QROWS, HD)]),
                load(wv.at[l], wqkv.at[l, pl.ds(QROWS + HD, HD)]), load(wv.at[l], wqkv.at[l, pl.ds(QROWS + 2 * HD, HD)])]

    first = [load(xp, vx.at[pl.ds(0, PIECE)]), load(an, van.at[:, pl.ds(0, D)])] + load_qkv(0)
    my_pos = pl.multiple_of(me * PIECE, PIECE)
    first += [load(cs.at[pl.ds(my_pos, PIECE)], vcs.at[pl.ds(0, PIECE)]), load(sn.at[pl.ds(my_pos, PIECE)], vsn.at[pl.ds(0, PIECE)])]
    second = [load(xr, vx.at[pl.ds(PIECE, RESP)]), load(cs.at[pl.ds(PROMPT, RESP)], vcs.at[pl.ds(PIECE, RESP)]),
              load(sn.at[pl.ds(PROMPT, RESP)], vsn.at[pl.ds(PIECE, RESP)])]

    barrier = pltpu.get_barrier_semaphore()
    pl.semaphore_signal(barrier, inc=1, device_id=y_peer, device_id_type=pl.DeviceIdType.MESH)
    for k in range(1, GROUP):
        pl.semaphore_signal(barrier, inc=1, device_id={'resp': lax.rem(me + k, GROUP)}, device_id_type=pl.DeviceIdType.MESH)
    pl.semaphore_wait(barrier, GROUP)

    def wo_slot(l, q, piece):
        start, size = WO_PIECES[piece]
        return woot.at[l, pl.ds(pl.multiple_of(q * WO_QUARTER + start, 16), size)]

    def wo_over_y(l):
        cps = []
        for start, size in WO_PIECES:
            rows = pl.ds(pl.multiple_of(me * WO_QUARTER + start, 16), size)
            cps.append(send(remote(wo.at[l, rows], woot.at[l, rows], y_peer)))
        return cps

    def wo_relay_own(l, piece, y_copy):
        y_copy.wait_recv()
        slot = wo_slot(l, me, piece)
        return send(remote(slot, slot, x_peer)), send(remote(slot, slot, d_peer))

    def wo_relay_x(l, piece, x_copy):
        x_copy.wait_recv()
        slot = wo_slot(l, lax.rem(me + 2, 4), piece)
        return send(remote(slot, slot, d_peer))

    wo_y0 = wo_over_y(0)

    zeros = jnp.zeros((512 - QROWS, D), BF16)
    for l in range(2):
        womy[l, QROWS:512] = zeros
        woot[l, QROWS:512] = zeros

    for cp in first:
        cp.wait()

    def halves(src, dst, l, rows):
        h = rows // 2
        return [load(src.at[l, pl.ds(0, h)], dst.at[l, pl.ds(0, h)]), load(src.at[l, pl.ds(h, h)], dst.at[l, pl.ds(h, h)])]

    lane = lax.broadcasted_iota(jnp.int32, (1, 128), 1)
    lo_head = lane < HD
    lo_half = lax.rem(lane, HD) < (HD // 2)

    def project(l, row0, n, hidden, kv_row):
        y = mm_t(hidden, wqkv[l])
        cos, sin = vcs[row0:row0 + n], vsn[row0:row0 + n]
        roped = []
        for j in range(4):
            b = y[:, 128 * j:128 * (j + 1)]
            partner = jnp.where(lo_half, pltpu.roll(b, 128 - HD // 2, 1), pltpu.roll(b, HD // 2, 1))
            roped.append(b * cos + partner * sin)
            qb[row0:row0 + n, 128 * j:128 * (j + 1)] = roped[-1].astype(BF16)
        kv[l, pl.ds(kv_row, n)] = jnp.where(lo_head, y[:, 512:640], roped[3]).astype(BF16)

    def share_kv(l):
        slot = kv.at[l, pl.ds(my_pos, PIECE)]
        return [send(remote(slot, slot, {'resp': lax.rem(me + k, GROUP)})) for k in range(1, GROUP)]

    def a_base(row0):
        return row0 * 7 // 2

    def attend(l, c, base, nk):
        row0, n = CHUNKS[c]
        kv_f = kv[l, 0:nk].astype(F32)
        kv_r = pltpu.roll(kv_f, HD, 1)
        k_even = jnp.where(lo_head, kv_r, 0.0).astype(BF16)
        k_odd = jnp.where(lo_head, 0.0, kv_f).astype(BF16)
        v_even = jnp.where(lo_head, kv_f, 0.0).astype(BF16)
        v_odd = jnp.where(lo_head, 0.0, kv_r).astype(BF16)
        q = [qb[row0:row0 + n, 128 * j:128 * (j + 1)] for j in range(4)]
        s_even = mm_t(jnp.concatenate(q, axis=0), k_even)
        s_odd = mm_t(jnp.concatenate(q[:3], axis=0), k_odd)
        vis = max(nk - n, 0) if c else 0
        keep = (lax.broadcasted_iota(jnp.int32, (n, nk - vis), 1) + vis) <= (base + lax.broadcasted_iota(jnp.int32, (n, nk - vis), 0))

        def probs(s):
            tail = jnp.where(keep, s[:, vis:], NEG_BIG)
            s = jnp.concatenate([s[:, :vis], tail], axis=1) if vis else tail
            top = jnp.max(s, axis=-1, keepdims=True)
            e = jnp.exp2((s - top) * (math.log2(math.e) / math.sqrt(HD)))
            return (e * (1.0 / jnp.sum(e, axis=-1, keepdims=True))).astype(BF16)

        p_even = jnp.concatenate([probs(s_even[j * n:(j + 1) * n]) for j in range(4)], axis=0)
        p_odd = jnp.concatenate([probs(s_odd[j * n:(j + 1) * n]) for j in range(3)], axis=0)
        o_even = mm(p_even, v_even)
        o_odd = mm(p_odd, v_odd)
        ab = a_base(row0)
        for j in range(3):
            blk = (o_even[j * n:(j + 1) * n] + o_odd[j * n:(j + 1) * n]).astype(BF16)
            amine[row0:row0 + n, 128 * j:128 * (j + 1)] = blk
            asnd[l, ab + j * n:ab + (j + 1) * n] = blk
        last = o_even[3 * n:4 * n]
        amine[row0:row0 + n, 384:512] = last.astype(BF16)
        asnd[l, ab + 3 * n:ab + 7 * n // 2] = (last[:n // 2] + pltpu.roll(last[n // 2:], HD, 1)).astype(BF16)
        rows = pl.ds(ab, 7 * n // 2)
        return send(remote(asnd.at[l, rows], arcv.at[l, rows], y_peer))

    def merge_attention(l, c, x_ref, a_copy):
        row0, n = CHUNKS[c]
        a_copy.wait_recv()
        ab = a_base(row0)
        packed = arcv[l, ab + 3 * n:ab + 7 * n // 2].astype(F32)
        last = jnp.concatenate([packed, pltpu.roll(packed, HD, 1)], axis=0).astype(BF16)
        a_oth = jnp.concatenate([arcv[l, ab + j * n:ab + (j + 1) * n] for j in range(3)] + [last], axis=1)
        proj = mm(amine[row0:row0 + n], womy[l]) + mm(a_oth, woot[l])
        xm[row0:row0 + n] = (x_ref[row0:row0 + n].astype(F32) + proj).astype(BF16)

    def mlp(l, c):
        row0, n = CHUNKS[c]
        g = rms(xm[row0:row0 + n].astype(F32), vmn[l:l + 1, 0:D])
        for b0, bn in FF_BLOCKS:
            gate = mm(g, vg[l, :, b0:b0 + bn])
            up = mm(g, vu[l, :, b0:b0 + bn])
            ub[0:n, b0:b0 + bn] = (gate * (1.0 / (1.0 + jnp.exp(-gate))) * up).astype(BF16)
        part[l, row0:row0 + n] = mm(ub[0:n], vd[l])
        h = n // 2
        src = part.at[l, pl.ds(pl.multiple_of(row0 + other * h, 16), h)]
        return send(remote(src, prcv.at[l, pl.ds(row0 // 2, h)], y_peer))

    def home_rows(c):
        row0, n = CHUNKS[c]
        return pl.ds(pl.multiple_of(row0 + side * (n // 2), 16), n // 2)

    def home_sum(l, c, p_copy):
        row0, n = CHUNKS[c]
        rows = home_rows(c)
        p_copy.wait_recv()
        total = part[l, rows] + prcv[l, row0 // 2:row0 // 2 + n // 2]
        return (xm[rows].astype(F32) + total).astype(BF16)

    def close_layer0(c, p_copy):
        rows = home_rows(c)
        x1[rows] = home_sum(0, c, p_copy)
        return send(remote(x1.at[rows], x1.at[rows], y_peer))

    def close_layer1(c, p_copy):
        rows = home_rows(c)
        hb[rows] = rms(home_sum(1, c, p_copy).astype(F32), vfn[:, 0:D])
        return send(remote(hb.at[rows], hb.at[rows], y_peer))

    def head(c, h_copy):
        row0, n = CHUNKS[c]
        t0 = row0 - PIECE
        h_copy.wait_recv()
        hidden = hb[row0:row0 + n]
        want = jnp.broadcast_to(vtgt[0:1, t0:t0 + n].astype(F32), (128, n)).T.astype(jnp.int32)[:, 0:1]
        top = None
        picked = None
        for b in range(4):
            lg = mm(hidden, vh[:, 512 * b:512 * (b + 1)])
            lgt[:, 512 * b:512 * (b + 1)] = lg
            ids = side * VOC + 512 * b + lax.broadcasted_iota(jnp.int32, (n, 512), 1)
            hit = jnp.where(ids == want, lg, 0.0)
            part_top = jnp.max(lg, axis=-1, keepdims=True)
            part_hit = jnp.sum(hit, axis=-1, keepdims=True)
            top = part_top if top is None else jnp.maximum(top, part_top)
            picked = part_hit if picked is None else picked + part_hit
        total = jnp.sum(jnp.exp(lgt[...] - top), axis=-1, keepdims=True)
        table = jnp.where(lane == 0, top, jnp.where(lane == 1, total, picked))
        st_s[c - 1] = table.T[0:8]
        return send(remote(st_s.at[c - 1], st_r.at[c - 1], y_peer))

    def finish(c, s_copy):
        row0, n = CHUNKS[c]
        s_copy.wait_recv()
        a, b = st_s[c - 1], st_r[c - 1]
        top = jnp.maximum(a[0:1], b[0:1])
        total = a[1:2] * jnp.exp(a[0:1] - top) + b[1:2] * jnp.exp(b[0:1] - top)
        out[0:1, row0 - PIECE:row0 - PIECE + n] = (a[2:3] + b[2:3]) - (top + jnp.log(total))

    hidden_p = rms(vx[0:PIECE].astype(F32), van[0:1, 0:D])
    project(0, 0, PIECE, hidden_p, my_pos)
    kv_cps = share_kv(0)
    for cp in second:
        cp.wait()
    w_my0 = [load(wo.at[0], womy.at[0, pl.ds(0, QROWS)]), load(mn, vmn.at[:, pl.ds(0, D)])]
    w_mlp0 = halves(wg, vg, 0, D) + halves(wu, vu, 0, D) + halves(wd, vd, 0, FF)
    project(0, PIECE, RESP, rms(vx[PIECE:ROWS].astype(F32), van[0:1, 0:D]), PROMPT)
    w_qkv1 = load_qkv(1)
    w_my1 = [load(wo.at[1], womy.at[1, pl.ds(0, QROWS)])]
    w_mlp1 = halves(wg, vg, 1, D) + halves(wu, vu, 1, D) + halves(wd, vd, 1, FF)
    w_head = [load(wh.at[pl.ds(0, D // 2)], vh.at[pl.ds(0, D // 2)]), load(wh.at[pl.ds(D // 2, D // 2)], vh.at[pl.ds(D // 2, D // 2)]),
              load(tgt, vtgt), load(fn, vfn.at[:, pl.ds(0, D)])]
    for cp in kv_cps:
        cp.wait_recv()
    a_cps = [attend(0, 0, my_pos, PROMPT), attend(0, 1, PROMPT, 384)]
    own0 = wo_relay_own(0, 0, wo_y0[0])
    a_cps.append(attend(0, 2, 384, 512))
    own1 = wo_relay_own(0, 1, wo_y0[1])
    d0 = wo_relay_x(0, 0, own0[0])
    wo_y1 = wo_over_y(1)
    d1 = wo_relay_x(0, 1, own1[0])
    for cp in w_my0 + w_mlp0:
        cp.wait()
    for cp in (own0[1], own1[1], d0, d1):
        cp.wait_recv()

    merge_attention(0, 0, vx, a_cps[0])
    p_p = mlp(0, 0)
    merge_attention(0, 1, vx, a_cps[1])
    p_1 = mlp(0, 1)
    x_p = close_layer0(0, p_p)
    merge_attention(0, 2, vx, a_cps[2])
    p_2 = mlp(0, 2)
    own0 = wo_relay_own(1, 0, wo_y1[0])
    own1 = wo_relay_own(1, 1, wo_y1[1])
    for cp in w_qkv1:
        cp.wait()
    x_1 = close_layer0(1, p_1)
    x_p.wait_recv()
    project(1, 0, PIECE, rms(x1[0:PIECE].astype(F32), van[1:2, 0:D]), my_pos)
    kv_cps = share_kv(1)
    d0 = wo_relay_x(1, 0, own0[0])
    d1 = wo_relay_x(1, 1, own1[0])
    x_2 = close_layer0(2, p_2)

    x_1.wait_recv()
    project(1, 64, 128, rms(x1[64:192].astype(F32), van[1:2, 0:D]), PROMPT)
    for cp in kv_cps:
        cp.wait_recv()
    a_1 = attend(1, 1, PROMPT, 384)
    x_2.wait_recv()
    project(1, 192, 128, rms(x1[192:320].astype(F32), van[1:2, 0:D]), PROMPT + 128)
    a_2 = attend(1, 2, 384, 512)
    for cp in w_my1 + w_mlp1 + w_head:
        cp.wait()
    for cp in (own0[1], own1[1], d0, d1):
        cp.wait_recv()
    merge_attention(1, 1, x1, a_1)
    p_1 = mlp(1, 1)
    merge_attention(1, 2, x1, a_2)
    p_2 = mlp(1, 2)
    h_1 = close_layer1(1, p_1)
    h_2 = close_layer1(2, p_2)
    s_1 = head(1, h_1)
    s_2 = head(2, h_2)
    finish(1, s_1)
    finish(2, s_2)
    for cp in sent:
        cp.wait_send()


def solution(mesh):
    rows_spec = P(('prompts', 'resp'), None)
    in_specs = (rows_spec, P(('prompts', 'resp'), None, None), rows_spec, P(), P(),
                P(None, None, 'model', None), P(None, None, 'model', None), P(None, None, 'model', None),
                P(None, 'model', None, None), P(None, None, 'model'), P(None, None, 'model'),
                P(None, 'model', None), P(), P(None, 'model'))
    cos, sin = rope_constants()

    def local_pass(x_piece, x_own, tgt_own, attn_norm, mlp_norm, w_q, w_k, w_v, w_o, w_gate, w_up, w_down, final_norm, w_head):
        def rows_first(w):
            return jnp.transpose(w, (0, 2, 3, 1)).reshape(2, w.shape[2] * HD, D)

        any_spec = pl.BlockSpec(memory_space=pl.ANY)
        scratch = [
            pltpu.VMEM((ROWS, D), BF16), pltpu.VMEM((ROWS, 128), F32), pltpu.VMEM((ROWS, 128), F32), pltpu.VMEM((1, RESP), jnp.int32),
            pltpu.VMEM((2, GAIN_PAD), F32), pltpu.VMEM((2, GAIN_PAD), F32), pltpu.VMEM((1, GAIN_PAD), F32),
            pltpu.VMEM((2, 640, D), BF16), pltpu.VMEM((2, 512, D), BF16), pltpu.VMEM((2, 512, D), BF16),
            pltpu.VMEM((2, D, FF), BF16), pltpu.VMEM((2, D, FF), BF16), pltpu.VMEM((2, FF, D), BF16), pltpu.VMEM((D, VOC), BF16),
            pltpu.VMEM((2, PROMPT + RESP, 128), BF16), pltpu.VMEM((ROWS, 512), BF16), pltpu.VMEM((ROWS, 512), BF16),
            pltpu.VMEM((2, ROWS * 7 // 2, 128), BF16), pltpu.VMEM((2, ROWS * 7 // 2, 128), BF16),
            pltpu.VMEM((ROWS, D), BF16), pltpu.VMEM((128, FF), BF16),
            pltpu.VMEM((2, ROWS, D), F32), pltpu.VMEM((2, ROWS // 2, D), F32),
            pltpu.VMEM((ROWS, D), BF16), pltpu.VMEM((ROWS, D), BF16), pltpu.VMEM((128, VOC), F32),
            pltpu.VMEM((2, 8, 128), F32), pltpu.VMEM((2, 8, 128), F32),
            pltpu.SemaphoreType.DMA((48,)), pltpu.SemaphoreType.DMA((48,)), pltpu.SemaphoreType.DMA((48,)),
        ]
        return pl.pallas_call(
            kernel,
            out_shape=jax.ShapeDtypeStruct((1, RESP), F32),
            in_specs=[any_spec] * 16,
            out_specs=pl.BlockSpec(memory_space=pltpu.VMEM),
            scratch_shapes=scratch,
            compiler_params=pltpu.CompilerParams(collective_id=0, has_side_effects=True, vmem_limit_bytes=67043328),
        )(x_piece, x_own[0], tgt_own, attn_norm, mlp_norm, rows_first(w_q), rows_first(w_k), rows_first(w_v),
          w_o.reshape(2, QROWS, D), w_gate, w_up, w_down, final_norm[None, :], w_head, jnp.asarray(cos), jnp.asarray(sin))

    return jax.shard_map(local_pass, mesh=mesh, in_specs=in_specs, out_specs=rows_spec, check_vma=False)
```

```python
import functools
import math

import jax
import jax.numpy as jnp
import numpy as np
from jax import lax
from jax.experimental import pallas as pl
from jax.experimental.pallas import tpu as pltpu
from jax.sharding import PartitionSpec as P

RMS_EPS = 1e-6
ROPE_BASE = 10000.0
NEG_BIG = -1e30
BF16 = jnp.bfloat16
F32 = jnp.float32

D = 896
HD = 64
PIECE = 64
RESP = 256
PROMPT = 256
ROWS = PIECE + RESP
FF = 2432
VOC = 2048
QROWS = 448
GROUP = 4
GAIN_PAD = 1024
C_P, C_1, C_2, C_3 = (0, 64), (64, 64), (128, 128), (256, 64)
C_A = (0, 128)
WO_QUARTER = QROWS // GROUP
WO_PIECES = ((0, 16), (16, 32), (48, 32), (80, 32))
FF_BLOCKS = ((0, 512), (512, 512), (1024, 512), (1536, 512), (2048, 384))


def rope_constants():
    inv = np.exp(np.arange(0, HD, 2, dtype=np.float32) * np.float32(-math.log(ROPE_BASE) / HD)).astype(np.float32)
    ang = np.arange(PROMPT + RESP, dtype=np.float32)[:, None] * inv[None, :]
    cos, sin = np.cos(ang).astype(np.float32), np.sin(ang).astype(np.float32)
    return np.concatenate([cos] * 4, axis=1), np.concatenate([-sin, sin] * 2, axis=1)


def mm(a, b):
    return jnp.dot(a, b, preferred_element_type=F32)


def mm_t(a, b):
    return lax.dot_general(a, b, (((1,), (1,)), ((), ())), preferred_element_type=F32)


def rms(x_f, gain):
    mean_sq = jnp.mean(x_f * x_f, axis=-1, keepdims=True)
    return (x_f * lax.rsqrt(mean_sq + RMS_EPS) * gain).astype(BF16)


def kernel(xp, xr, tgt, an, mn, wq, wk, wv, wo, wg, wu, wd, fn, wh, cs, sn, out,
           vx, vcs, vsn, vtgt, van, vmn, vfn, wqkv, womy, woot, vg, vu, vd, vh,
           kv, qb, amine, mo, asnd, arcv, xm, ub, part, prcv, x1, hb, lgt, st_s, st_r,
           lsem, ssem, rsem):
    me = lax.axis_index('resp')
    side = lax.axis_index('model')
    other = 1 - side
    y_peer = {'model': other}
    d_peer = {'resp': me + 1 - 2 * lax.rem(me, 2)}
    x_peer = {'resp': lax.rem(me + 2, 4)}

    counts = {'l': 0, 'r': 0}

    def load(src, dst):
        cp = pltpu.make_async_copy(src, dst, lsem.at[counts['l']])
        counts['l'] += 1
        cp.start()
        return cp

    def remote(src, dst, peer):
        k = counts['r']
        counts['r'] += 1
        return pltpu.make_async_remote_copy(src_ref=src, dst_ref=dst, send_sem=ssem.at[k], recv_sem=rsem.at[k],
                                            device_id=peer, device_id_type=pl.DeviceIdType.MESH)

    sent = []

    def send(cp):
        cp.start()
        sent.append(cp)
        return cp

    def load_qkv(l):
        return [load(wq.at[l], wqkv.at[l, pl.ds(0, QROWS)]), load(wk.at[l], wqkv.at[l, pl.ds(QROWS, HD)]),
                load(wv.at[l], wqkv.at[l, pl.ds(QROWS + HD, HD)]), load(wv.at[l], wqkv.at[l, pl.ds(QROWS + 2 * HD, HD)])]

    first = [load(xp, vx.at[pl.ds(0, PIECE)]), load(an, van.at[:, pl.ds(0, D)])] + load_qkv(0)
    my_pos = pl.multiple_of(me * PIECE, PIECE)
    first += [load(cs.at[pl.ds(my_pos, PIECE)], vcs.at[pl.ds(0, PIECE)]), load(sn.at[pl.ds(my_pos, PIECE)], vsn.at[pl.ds(0, PIECE)])]
    second = [load(xr, vx.at[pl.ds(PIECE, RESP)]), load(cs.at[pl.ds(PROMPT, RESP)], vcs.at[pl.ds(PIECE, RESP)]),
              load(sn.at[pl.ds(PROMPT, RESP)], vsn.at[pl.ds(PIECE, RESP)])]

    barrier = pltpu.get_barrier_semaphore()
    pl.semaphore_signal(barrier, inc=1, device_id=y_peer, device_id_type=pl.DeviceIdType.MESH)
    for k in range(1, GROUP):
        pl.semaphore_signal(barrier, inc=1, device_id={'resp': lax.rem(me + k, GROUP)}, device_id_type=pl.DeviceIdType.MESH)
    pl.semaphore_wait(barrier, GROUP)

    def wo_slot(l, q, piece):
        start, size = WO_PIECES[piece]
        return woot.at[l, pl.ds(pl.multiple_of(q * WO_QUARTER + start, 16), size)]

    def wo_over_y(l):
        cps = []
        for start, size in WO_PIECES:
            rows = pl.ds(pl.multiple_of(me * WO_QUARTER + start, 16), size)
            cps.append(send(remote(wo.at[l, rows], woot.at[l, rows], y_peer)))
        return cps

    def wo_relay_own(l, piece, y_copy):
        y_copy.wait_recv()
        slot = wo_slot(l, me, piece)
        return send(remote(slot, slot, x_peer)), send(remote(slot, slot, d_peer))

    def wo_relay_x(l, piece, x_copy):
        x_copy.wait_recv()
        slot = wo_slot(l, lax.rem(me + 2, 4), piece)
        return send(remote(slot, slot, d_peer))

    wo_y0 = wo_over_y(0)

    zeros = jnp.zeros((512 - QROWS, D), BF16)
    for l in range(2):
        womy[l, QROWS:512] = zeros
        woot[l, QROWS:512] = zeros
    kv[1, PROMPT:PROMPT + RESP] = jnp.zeros((RESP, 128), BF16)

    for cp in first:
        cp.wait()

    def halves(src, dst, l, rows):
        h = rows // 2
        return [load(src.at[l, pl.ds(0, h)], dst.at[l, pl.ds(0, h)]), load(src.at[l, pl.ds(h, h)], dst.at[l, pl.ds(h, h)])]

    lane = lax.broadcasted_iota(jnp.int32, (1, 128), 1)
    lo_head = lane < HD
    lo_half = lax.rem(lane, HD) < (HD // 2)

    def project(l, row0, n, hidden, kv_rows):
        y = mm_t(hidden, wqkv[l])
        cos, sin = vcs[row0:row0 + n], vsn[row0:row0 + n]
        roped = []
        for j in range(4):
            b = y[:, 128 * j:128 * (j + 1)]
            partner = jnp.where(lo_half, pltpu.roll(b, 128 - HD // 2, 1), pltpu.roll(b, HD // 2, 1))
            roped.append(b * cos + partner * sin)
            qb[row0:row0 + n, 128 * j:128 * (j + 1)] = roped[-1].astype(BF16)
        pair = jnp.where(lo_head, y[:, 512:640], roped[3]).astype(BF16)
        step = n // len(kv_rows)
        for k, kv_row in enumerate(kv_rows):
            kv[l, pl.ds(kv_row, step)] = pair[k * step:(k + 1) * step]

    def share_kv(l):
        slot = kv.at[l, pl.ds(my_pos, PIECE)]
        return [send(remote(slot, slot, {'resp': lax.rem(me + k, GROUP)})) for k in range(1, GROUP)]

    def a_base(row0):
        return row0 * 7 // 2

    def attend(l, chunk, base, vis, nk):
        row0, n = chunk
        kv_f = kv[l, 0:nk].astype(F32)
        kv_r = pltpu.roll(kv_f, HD, 1)
        k_even = jnp.where(lo_head, kv_r, 0.0).astype(BF16)
        k_odd = jnp.where(lo_head, 0.0, kv_f).astype(BF16)
        v_even = jnp.where(lo_head, kv_f, 0.0).astype(BF16)
        v_odd = jnp.where(lo_head, 0.0, kv_r).astype(BF16)
        q = [qb[row0:row0 + n, 128 * j:128 * (j + 1)] for j in range(4)]
        s_even = mm_t(jnp.concatenate(q, axis=0), k_even)
        s_odd = mm_t(jnp.concatenate(q[:3], axis=0), k_odd)
        keep = (lax.broadcasted_iota(jnp.int32, (n, nk - vis), 1) + vis) <= (base + lax.broadcasted_iota(jnp.int32, (n, nk - vis), 0))

        def probs(s):
            tail = jnp.where(keep, s[:, vis:], NEG_BIG)
            s = jnp.concatenate([s[:, :vis], tail], axis=1) if vis else tail
            top = jnp.max(s, axis=-1, keepdims=True)
            e = jnp.exp2((s - top) * (math.log2(math.e) / math.sqrt(HD)))
            return (e * (1.0 / jnp.sum(e, axis=-1, keepdims=True))).astype(BF16)

        p_even = jnp.concatenate([probs(s_even[j * n:(j + 1) * n]) for j in range(4)], axis=0)
        p_odd = jnp.concatenate([probs(s_odd[j * n:(j + 1) * n]) for j in range(3)], axis=0)
        o_even = mm(p_even, v_even)
        o_odd = mm(p_odd, v_odd)
        ab = a_base(row0)
        for j in range(3):
            blk = (o_even[j * n:(j + 1) * n] + o_odd[j * n:(j + 1) * n]).astype(BF16)
            amine[row0:row0 + n, 128 * j:128 * (j + 1)] = blk
            asnd[l, ab + j * n:ab + (j + 1) * n] = blk
        last = o_even[3 * n:4 * n]
        amine[row0:row0 + n, 384:512] = last.astype(BF16)
        asnd[l, ab + 3 * n:ab + 7 * n // 2] = (last[:n // 2] + pltpu.roll(last[n // 2:], HD, 1)).astype(BF16)
        rows = pl.ds(ab, 7 * n // 2)
        return send(remote(asnd.at[l, rows], arcv.at[l, rows], y_peer))

    def merge_own(l, chunk):
        row0, n = chunk
        mo[row0:row0 + n] = mm(amine[row0:row0 + n], womy[l])

    def received(l, chunk):
        row0, n = chunk
        ab = a_base(row0)
        packed = arcv[l, ab + 3 * n:ab + 7 * n // 2].astype(F32)
        last = jnp.concatenate([packed, pltpu.roll(packed, HD, 1)], axis=0).astype(BF16)
        return jnp.concatenate([arcv[l, ab + j * n:ab + (j + 1) * n] for j in range(3)] + [last], axis=1)

    def merge_attention(l, chunk, x_ref, parts):
        row0, n = chunk
        a_oth = jnp.concatenate([received(l, p) for p in parts], axis=0)
        proj = mo[row0:row0 + n] + mm(a_oth, woot[l])
        xm[row0:row0 + n] = (x_ref[row0:row0 + n].astype(F32) + proj).astype(BF16)

    def mlp(l, chunk):
        row0, n = chunk
        g = rms(xm[row0:row0 + n].astype(F32), vmn[l:l + 1, 0:D])
        for b0, bn in FF_BLOCKS:
            gate = mm(g, vg[l, :, b0:b0 + bn])
            up = mm(g, vu[l, :, b0:b0 + bn])
            ub[0:n, b0:b0 + bn] = (gate * (1.0 / (1.0 + jnp.exp(-gate))) * up).astype(BF16)
        part[l, row0:row0 + n] = mm(ub[0:n], vd[l])
        h = n // 2
        src = part.at[l, pl.ds(pl.multiple_of(row0 + other * h, 16), h)]
        return remote(src, prcv.at[l, pl.ds(row0 // 2, h)], y_peer)

    def home_rows(chunk):
        row0, n = chunk
        return pl.ds(pl.multiple_of(row0 + side * (n // 2), 16), n // 2)

    def home_sum(l, chunk):
        row0, n = chunk
        rows = home_rows(chunk)
        total = part[l, rows] + prcv[l, row0 // 2:row0 // 2 + n // 2]
        return (xm[rows].astype(F32) + total).astype(BF16)

    def close_layer0(chunk):
        rows = home_rows(chunk)
        x1[rows] = home_sum(0, chunk)
        return send(remote(x1.at[rows], x1.at[rows], y_peer))

    def close_layer1(chunk):
        rows = home_rows(chunk)
        hb[rows] = rms(home_sum(1, chunk).astype(F32), vfn[...].reshape(1, GAIN_PAD)[:, 0:D])
        return send(remote(hb.at[rows], hb.at[rows], y_peer))

    def head(k, chunk):
        row0, n = chunk
        t0 = row0 - PIECE
        hidden = hb[row0:row0 + n]
        want = jnp.broadcast_to(vtgt[0:1, t0:t0 + n].astype(F32), (128, n)).T.astype(jnp.int32)[:, 0:1]
        top = None
        picked = None
        for b in range(4):
            lg = mm(hidden, vh[:, 512 * b:512 * (b + 1)])
            lgt[0:n, 512 * b:512 * (b + 1)] = lg
            ids = side * VOC + 512 * b + lax.broadcasted_iota(jnp.int32, (n, 512), 1)
            hit = jnp.where(ids == want, lg, 0.0)
            part_top = jnp.max(lg, axis=-1, keepdims=True)
            part_hit = jnp.sum(hit, axis=-1, keepdims=True)
            top = part_top if top is None else jnp.maximum(top, part_top)
            picked = part_hit if picked is None else picked + part_hit
        total = jnp.sum(jnp.exp(lgt[0:n] - top), axis=-1, keepdims=True)
        table = jnp.where(lane == 0, top, jnp.where(lane == 1, total, picked))
        st_s[k, :, 0:n] = table.T[0:8]
        return send(remote(st_s.at[k], st_r.at[k], y_peer))

    def finish(k, chunk):
        row0, n = chunk
        a, b = st_s[k, :, 0:n], st_r[k, :, 0:n]
        top = jnp.maximum(a[0:1], b[0:1])
        total = a[1:2] * jnp.exp(a[0:1] - top) + b[1:2] * jnp.exp(b[0:1] - top)
        out[0:1, row0 - PIECE:row0 - PIECE + n] = (a[2:3] + b[2:3]) - (top + jnp.log(total))

    scope = jax.named_scope

    def wait(*cps):
        for cp in cps:
            cp.wait_recv()

    with scope('proj_p'):
        project(0, 0, PIECE, rms(vx[0:PIECE].astype(F32), van[0:1, 0:D]), (my_pos,))
        kv_cps = share_kv(0)
    with scope('wait_x'):
        for cp in second:
            cp.wait()
        w_my0 = [load(wo.at[0], womy.at[0, pl.ds(0, QROWS)]), load(mn, vmn.at[:, pl.ds(0, D)])]
        w_mlp0 = halves(wg, vg, 0, D) + halves(wu, vu, 0, D) + halves(wd, vd, 0, FF)
    with scope('proj_r'):
        project(0, PIECE, RESP, rms(vx[PIECE:ROWS].astype(F32), van[0:1, 0:D]), (PROMPT,))
    w_qkv1 = load_qkv(1)
    w_my1 = [load(wo.at[1], womy.at[1, pl.ds(0, QROWS)])]
    w_mlp1 = halves(wg, vg, 1, D) + halves(wu, vu, 1, D) + halves(wd, vd, 1, FF)
    w_head = [load(wh.at[pl.ds(0, D // 2)], vh.at[pl.ds(0, D // 2)]), load(wh.at[pl.ds(D // 2, D // 2)], vh.at[pl.ds(D // 2, D // 2)]),
              load(tgt, vtgt), load(fn, vfn.at[pl.ds(0, D)])]
    with scope('wait_kv0'):
        wait(*kv_cps)
    own = []
    with scope('relay0_0'):
        own.append(wo_relay_own(0, 0, wo_y0[0]))
    with scope('att0_p'):
        a_p = attend(0, C_P, my_pos, 0, PROMPT)
    with scope('att0_1'):
        a_1 = attend(0, C_1, 256, 256, 384)
    with scope('relay0_1'):
        own.append(wo_relay_own(0, 1, wo_y0[1]))
    with scope('att0_2'):
        a_2 = attend(0, C_2, 320, 256, 512)
    with scope('relay0_2'):
        own.append(wo_relay_own(0, 2, wo_y0[2]))
    with scope('att0_3'):
        a_3 = attend(0, C_3, 448, 384, 512)
    with scope('relay0_3'):
        own.append(wo_relay_own(0, 3, wo_y0[3]))
        wo_y1 = wo_over_y(1)
    with scope('relay0_x0'):
        dd = [wo_relay_x(0, 0, own[0][0])]
    with scope('own0'):
        for cp in w_my0:
            cp.wait()
        for ch in (C_A, C_2, C_3):
            merge_own(0, ch)
    with scope('relay0_x123'):
        dd += [wo_relay_x(0, k, own[k][0]) for k in range(1, 4)]
    with scope('wait_w0'):
        for cp in w_mlp0:
            cp.wait()
    with scope('wait_wo0'):
        wait(*[o[1] for o in own], *dd)

    with scope('wait_a0_a'):
        wait(a_p, a_1)
    with scope('merge0_a'):
        merge_attention(0, C_A, vx, (C_P, C_1))
    with scope('mlp0_a'):
        p_a = send(mlp(0, C_A))
    with scope('wait_a0_2'):
        wait(a_2)
    with scope('merge0_2'):
        merge_attention(0, C_2, vx, (C_2,))
    with scope('mlp0_2'):
        p_2 = send(mlp(0, C_2))
    with scope('wait_a0_3'):
        wait(a_3)
    with scope('merge0_3'):
        merge_attention(0, C_3, vx, (C_3,))
    with scope('mlp0_3'):
        p_3 = mlp(0, C_3)
    with scope('relay1'):
        own = [wo_relay_own(1, k, wo_y1[k]) for k in range(4)]
        for cp in w_qkv1:
            cp.wait()
    with scope('wait_p0_a'):
        wait(p_a)
    with scope('close0_a'):
        x_a = close_layer0(C_A)
        send(p_3)
    with scope('relay1_x'):
        dd = [wo_relay_x(1, k, own[k][0]) for k in range(4)]
    with scope('wait_p0_2'):
        wait(p_2)
    with scope('close0_2'):
        x_2 = close_layer0(C_2)
    with scope('wait_x_a'):
        wait(x_a)
    with scope('proj1_a'):
        project(1, 0, 128, rms(x1[0:128].astype(F32), van[1:2, 0:D]), (my_pos, PROMPT))
        kv_cps = share_kv(1)
    with scope('wait_p0_3'):
        wait(p_3)
    with scope('close0_3'):
        x_3 = close_layer0(C_3)

    with scope('wait_kv1'):
        wait(*kv_cps)
        for cp in w_my1:
            cp.wait()
    with scope('att1_1'):
        a_1 = attend(1, C_1, 256, 256, 384)
        merge_own(1, C_1)
    with scope('wait_x_2'):
        wait(x_2)
    with scope('proj1_2'):
        project(1, 128, 128, rms(x1[128:256].astype(F32), van[1:2, 0:D]), (PROMPT + 64,))
    with scope('att1_2'):
        a_2 = attend(1, C_2, 320, 256, 512)
    with scope('wait_x_3'):
        wait(x_3)
    with scope('proj1_3'):
        project(1, 256, 64, rms(x1[256:320].astype(F32), van[1:2, 0:D]), (PROMPT + 192,))
    with scope('att1_3'):
        a_3 = attend(1, C_3, 448, 384, 512)
        merge_own(1, C_2)
    with scope('wait_w1'):
        for cp in w_mlp1 + w_head:
            cp.wait()
        wait(*[o[1] for o in own], *dd)
    with scope('wait_a1_1'):
        wait(a_1)
    with scope('merge1_1'):
        merge_attention(1, C_1, x1, (C_1,))
    with scope('mlp1_1'):
        p_1 = send(mlp(1, C_1))
    with scope('own1_3'):
        merge_own(1, C_3)
    with scope('wait_a1_2'):
        wait(a_2)
    with scope('merge1_2'):
        merge_attention(1, C_2, x1, (C_2,))
    with scope('mlp1_2'):
        p_2 = send(mlp(1, C_2))
    with scope('wait_a1_3'):
        wait(a_3)
    with scope('merge1_3'):
        merge_attention(1, C_3, x1, (C_3,))
    with scope('mlp1_3'):
        p_3 = mlp(1, C_3)
    with scope('wait_p1_1'):
        wait(p_1)
    with scope('close1_1'):
        h_1 = close_layer1(C_1)
        send(p_3)
    with scope('wait_p1_2'):
        wait(p_2)
    with scope('close1_2'):
        h_2 = close_layer1(C_2)
    with scope('wait_h_1'):
        wait(h_1)
    with scope('head_1'):
        s_1 = head(0, C_1)
    with scope('wait_p1_3'):
        wait(p_3)
    with scope('close1_3'):
        h_3 = close_layer1(C_3)
    with scope('wait_h_2'):
        wait(h_2)
    with scope('head_2'):
        s_2 = head(1, C_2)
    with scope('wait_h_3'):
        wait(h_3)
    with scope('head_3'):
        s_3 = head(2, C_3)
    with scope('wait_s'):
        wait(s_1, s_2, s_3)
    with scope('finish'):
        for k, ch in enumerate((C_1, C_2, C_3)):
            finish(k, ch)
    with scope('wait_sends'):
        for cp in sent:
            cp.wait_send()


def solution(mesh):
    rows_spec = P(('prompts', 'resp'), None)
    in_specs = (rows_spec, P(('prompts', 'resp'), None, None), rows_spec, P(), P(),
                P(None, None, 'model', None), P(None, None, 'model', None), P(None, None, 'model', None),
                P(None, 'model', None, None), P(None, None, 'model'), P(None, None, 'model'),
                P(None, 'model', None), P(), P(None, 'model'))
    cos, sin = rope_constants()

    def local_pass(x_piece, x_own, tgt_own, attn_norm, mlp_norm, w_q, w_k, w_v, w_o, w_gate, w_up, w_down, final_norm, w_head):
        def rows_first(w):
            return jnp.transpose(w, (0, 2, 3, 1)).reshape(2, w.shape[2] * HD, D)

        any_spec = pl.BlockSpec(memory_space=pl.ANY)
        scratch = [
            pltpu.VMEM((ROWS, D), BF16), pltpu.VMEM((ROWS, 128), F32), pltpu.VMEM((ROWS, 128), F32), pltpu.VMEM((1, RESP), jnp.int32),
            pltpu.VMEM((2, GAIN_PAD), F32), pltpu.VMEM((2, GAIN_PAD), F32), pltpu.VMEM((GAIN_PAD,), F32),
            pltpu.VMEM((2, 640, D), BF16), pltpu.VMEM((2, 512, D), BF16), pltpu.VMEM((2, 512, D), BF16),
            pltpu.VMEM((2, D, FF), BF16), pltpu.VMEM((2, D, FF), BF16), pltpu.VMEM((2, FF, D), BF16), pltpu.VMEM((D, VOC), BF16),
            pltpu.VMEM((2, PROMPT + RESP, 128), BF16), pltpu.VMEM((ROWS, 512), BF16), pltpu.VMEM((ROWS, 512), BF16), pltpu.VMEM((ROWS, D), F32),
            pltpu.VMEM((2, ROWS * 7 // 2, 128), BF16), pltpu.VMEM((2, ROWS * 7 // 2, 128), BF16),
            pltpu.VMEM((ROWS, D), BF16), pltpu.VMEM((128, FF), BF16),
            pltpu.VMEM((2, ROWS, D), F32), pltpu.VMEM((2, ROWS // 2, D), F32),
            pltpu.VMEM((ROWS, D), BF16), pltpu.VMEM((ROWS, D), BF16), pltpu.VMEM((128, VOC), F32),
            pltpu.VMEM((3, 8, 128), F32), pltpu.VMEM((3, 8, 128), F32),
            pltpu.SemaphoreType.DMA((48,)), pltpu.SemaphoreType.DMA((72,)), pltpu.SemaphoreType.DMA((72,)),
        ]
        return pl.pallas_call(
            kernel,
            out_shape=jax.ShapeDtypeStruct((1, RESP), F32),
            in_specs=[any_spec] * 16,
            out_specs=pl.BlockSpec(memory_space=pltpu.VMEM),
            scratch_shapes=scratch,
            compiler_params=pltpu.CompilerParams(collective_id=0, has_side_effects=True, vmem_limit_bytes=67043328),
        )(x_piece, x_own[0], tgt_own, attn_norm, mlp_norm, rows_first(w_q), rows_first(w_k), rows_first(w_v),
          w_o.reshape(2, QROWS, D), w_gate, w_up, w_down, final_norm, w_head, jnp.asarray(cos), jnp.asarray(sin))

    return jax.shard_map(local_pass, mesh=mesh, in_specs=in_specs, out_specs=rows_spec, check_vma=False)
```

```python
import functools
import math

import jax
import jax.numpy as jnp
import numpy as np
from jax import lax
from jax.experimental import pallas as pl
from jax.experimental.pallas import tpu as pltpu
from jax.sharding import PartitionSpec as P

RMS_EPS = 1e-6
ROPE_BASE = 10000.0
NEG_BIG = -1e30
BF16 = jnp.bfloat16
F32 = jnp.float32

D = 896
HD = 64
PIECE = 64
RESP = 256
PROMPT = 256
ROWS = PIECE + RESP
FF = 2432
VOC = 2048
QROWS = 448
GROUP = 4
GAIN_PAD = 1024
C_P, C_1, C_2, C_3 = (0, 64), (64, 64), (128, 128), (256, 64)
C_A = (0, 128)
WO_QUARTER = QROWS // GROUP
WO_PIECES = ((0, 16), (16, 32), (48, 32), (80, 32))
OUT_BLOCKS = ((0, 512), (512, 384))
FF_BLOCKS = ((0, 512), (512, 512), (1024, 512), (1536, 512), (2048, 384))


def rope_constants():
    inv = np.exp(np.arange(0, HD, 2, dtype=np.float32) * np.float32(-math.log(ROPE_BASE) / HD)).astype(np.float32)
    ang = np.arange(PROMPT + RESP, dtype=np.float32)[:, None] * inv[None, :]
    cos, sin = np.cos(ang).astype(np.float32), np.sin(ang).astype(np.float32)
    return np.concatenate([cos] * 4, axis=1), np.concatenate([-sin, sin] * 2, axis=1)


def mm(a, b):
    return jnp.dot(a, b, preferred_element_type=F32)


def mm_t(a, b):
    return lax.dot_general(a, b, (((1,), (1,)), ((), ())), preferred_element_type=F32)


def rms(x_f, gain):
    mean_sq = jnp.mean(x_f * x_f, axis=-1, keepdims=True)
    return (x_f * lax.rsqrt(mean_sq + RMS_EPS) * gain).astype(BF16)


def kernel(xp, xr, tgt, an, mn, wq, wk, wv, wo, wg, wu, wd, fn, wh, cs, sn, out,
           vx, vcs, vsn, vtgt, van, vmn, vfn, wqkv, womy, woot, vg, vu, vd, vh,
           kv, kx, wt1, want, qb, amine, mo, asnd, arcv, xm, ub, part, prcv, x1, hb, st_s, st_r,
           lsem, ssem, rsem):
    me = lax.axis_index('resp')
    side = lax.axis_index('model')
    other = 1 - side
    y_peer = {'model': other}
    d_peer = {'resp': me + 1 - 2 * lax.rem(me, 2)}
    x_peer = {'resp': lax.rem(me + 2, 4)}

    counts = {'l': 0, 'r': 0}

    def load(src, dst):
        cp = pltpu.make_async_copy(src, dst, lsem.at[counts['l']])
        counts['l'] += 1
        cp.start()
        return cp

    def remote(src, dst, peer):
        k = counts['r']
        counts['r'] += 1
        return pltpu.make_async_remote_copy(src_ref=src, dst_ref=dst, send_sem=ssem.at[k], recv_sem=rsem.at[k],
                                            device_id=peer, device_id_type=pl.DeviceIdType.MESH)

    sent = []

    def send(cp):
        cp.start()
        sent.append(cp)
        return cp

    def load_qkv(l):
        return [load(wq.at[l], wqkv.at[l, pl.ds(0, QROWS)]), load(wk.at[l], wqkv.at[l, pl.ds(QROWS, HD)]),
                load(wv.at[l], wqkv.at[l, pl.ds(QROWS + HD, HD)]), load(wv.at[l], wqkv.at[l, pl.ds(QROWS + 2 * HD, HD)])]

    first = [load(xp, vx.at[pl.ds(0, PIECE)]), load(an, van.at[:, pl.ds(0, D)])] + load_qkv(0)
    my_pos = pl.multiple_of(me * PIECE, PIECE)
    first += [load(cs.at[pl.ds(my_pos, PIECE)], vcs.at[pl.ds(0, PIECE)]), load(sn.at[pl.ds(my_pos, PIECE)], vsn.at[pl.ds(0, PIECE)])]
    second = [load(xr, vx.at[pl.ds(PIECE, RESP)]), load(cs.at[pl.ds(PROMPT, RESP)], vcs.at[pl.ds(PIECE, RESP)]),
              load(sn.at[pl.ds(PROMPT, RESP)], vsn.at[pl.ds(PIECE, RESP)])]

    barrier = pltpu.get_barrier_semaphore()
    pl.semaphore_signal(barrier, inc=1, device_id=y_peer, device_id_type=pl.DeviceIdType.MESH)
    for k in range(1, GROUP):
        pl.semaphore_signal(barrier, inc=1, device_id={'resp': lax.rem(me + k, GROUP)}, device_id_type=pl.DeviceIdType.MESH)
    pl.semaphore_wait(barrier, GROUP)

    def wo_slot(l, q, piece):
        start, size = WO_PIECES[piece]
        return woot.at[l, pl.ds(pl.multiple_of(q * WO_QUARTER + start, 16), size)]

    def wo_over_y(l):
        cps = []
        for start, size in WO_PIECES:
            rows = pl.ds(pl.multiple_of(me * WO_QUARTER + start, 16), size)
            cps.append(send(remote(wo.at[l, rows], woot.at[l, rows], y_peer)))
        return cps

    def wo_relay_own(l, piece, y_copy):
        y_copy.wait_recv()
        slot = wo_slot(l, me, piece)
        return send(remote(slot, slot, x_peer)), send(remote(slot, slot, d_peer))

    def wo_relay_x(l, piece, x_copy):
        x_copy.wait_recv()
        slot = wo_slot(l, lax.rem(me + 2, 4), piece)
        return send(remote(slot, slot, d_peer))

    wo_y0 = wo_over_y(0)

    zeros = jnp.zeros((512 - QROWS, D), BF16)
    for l in range(2):
        womy[l, QROWS:512] = zeros
        woot[l, QROWS:512] = zeros
    for k in range(4):
        kx[1, k, PROMPT:PROMPT + RESP] = jnp.zeros((RESP, 128), BF16)

    for cp in first:
        cp.wait()

    def halves(src, dst, l, rows):
        h = rows // 2
        return [load(src.at[l, pl.ds(0, h)], dst.at[l, pl.ds(0, h)]), load(src.at[l, pl.ds(h, h)], dst.at[l, pl.ds(h, h)])]

    lane = lax.broadcasted_iota(jnp.int32, (1, 128), 1)
    lo_head = lane < HD
    lo_half = lax.rem(lane, HD) < (HD // 2)

    def expand(l, row0, pair):
        f = pair.astype(F32)
        r = pltpu.roll(f, HD, 1)
        n = pair.shape[0]
        kx[l, 0, row0:row0 + n] = jnp.where(lo_head, r, 0.0).astype(BF16)
        kx[l, 1, row0:row0 + n] = jnp.where(lo_head, 0.0, f).astype(BF16)
        kx[l, 2, row0:row0 + n] = jnp.where(lo_head, f, 0.0).astype(BF16)
        kx[l, 3, row0:row0 + n] = jnp.where(lo_head, 0.0, r).astype(BF16)

    def project(l, row0, n, hidden, piece_rows):
        y = mm(hidden, wt1[...]) if l else mm_t(hidden, wqkv[l])
        cos, sin = vcs[row0:row0 + n], vsn[row0:row0 + n]
        roped = []
        for j in range(4):
            b = y[:, 128 * j:128 * (j + 1)]
            partner = jnp.where(lo_half, pltpu.roll(b, 128 - HD // 2, 1), pltpu.roll(b, HD // 2, 1))
            roped.append(b * cos + partner * sin)
            qb[row0:row0 + n, 128 * j:128 * (j + 1)] = roped[-1].astype(BF16)
        pair = jnp.where(lo_head, y[:, 512:640], roped[3]).astype(BF16)
        if piece_rows:
            kv[l, pl.ds(my_pos, PIECE)] = pair[0:PIECE]
        if n > piece_rows:
            expand(l, PROMPT + row0 + piece_rows - PIECE, pair[piece_rows:n])

    def share_kv(l):
        slot = kv.at[l, pl.ds(my_pos, PIECE)]
        return [send(remote(slot, slot, {'resp': lax.rem(me + k, GROUP)})) for k in range(1, GROUP)]

    def a_base(row0):
        return row0 * 7 // 2

    def attend(l, chunk, base, vis, nk):
        row0, n = chunk
        k_even, k_odd, v_even, v_odd = (kx[l, k, 0:nk] for k in range(4))
        q = [qb[row0:row0 + n, 128 * j:128 * (j + 1)] for j in range(4)]
        s_even = mm_t(jnp.concatenate(q, axis=0), k_even)
        s_odd = mm_t(jnp.concatenate(q[:3], axis=0), k_odd)
        keep = (lax.broadcasted_iota(jnp.int32, (n, nk - vis), 1) + vis) <= (base + lax.broadcasted_iota(jnp.int32, (n, nk - vis), 0))

        def probs(s):
            tail = jnp.where(keep, s[:, vis:], NEG_BIG)
            s = jnp.concatenate([s[:, :vis], tail], axis=1) if vis else tail
            top = jnp.max(s, axis=-1, keepdims=True)
            e = jnp.exp2((s - top) * (math.log2(math.e) / math.sqrt(HD)))
            return (e * (1.0 / jnp.sum(e, axis=-1, keepdims=True))).astype(BF16)

        p_even = jnp.concatenate([probs(s_even[j * n:(j + 1) * n]) for j in range(4)], axis=0)
        p_odd = jnp.concatenate([probs(s_odd[j * n:(j + 1) * n]) for j in range(3)], axis=0)
        o_even = mm(p_even, v_even)
        o_odd = mm(p_odd, v_odd)
        ab = a_base(row0)
        for j in range(3):
            blk = (o_even[j * n:(j + 1) * n] + o_odd[j * n:(j + 1) * n]).astype(BF16)
            amine[row0:row0 + n, 128 * j:128 * (j + 1)] = blk
            asnd[l, ab + j * n:ab + (j + 1) * n] = blk
        last = o_even[3 * n:4 * n]
        amine[row0:row0 + n, 384:512] = last.astype(BF16)
        asnd[l, ab + 3 * n:ab + 7 * n // 2] = (last[:n // 2] + pltpu.roll(last[n // 2:], HD, 1)).astype(BF16)
        rows = pl.ds(ab, 7 * n // 2)
        return send(remote(asnd.at[l, rows], arcv.at[l, rows], y_peer))

    def merge_own(l, chunk):
        row0, n = chunk
        mo[row0:row0 + n] = mm(amine[row0:row0 + n], womy[l])

    def received(l, chunk):
        row0, n = chunk
        ab = a_base(row0)
        packed = arcv[l, ab + 3 * n:ab + 7 * n // 2].astype(F32)
        last = jnp.concatenate([packed, pltpu.roll(packed, HD, 1)], axis=0).astype(BF16)
        return jnp.concatenate([arcv[l, ab + j * n:ab + (j + 1) * n] for j in range(3)] + [last], axis=1)

    def merge_attention(l, chunk, x_ref, parts):
        row0, n = chunk
        a_oth = jnp.concatenate([received(l, p) for p in parts], axis=0)
        proj = mo[row0:row0 + n] + mm(a_oth, woot[l])
        xm[row0:row0 + n] = (x_ref[row0:row0 + n].astype(F32) + proj).astype(BF16)

    def mlp(l, chunk, now=2):
        row0, n = chunk
        g = rms(xm[row0:row0 + n].astype(F32), vmn[l:l + 1, 0:D])
        for b0, bn in FF_BLOCKS:
            gate = mm(g, vg[l, :, b0:b0 + bn])
            up = mm(g, vu[l, :, b0:b0 + bn])
            ub[0:n, b0:b0 + bn] = (gate * (1.0 / (1.0 + jnp.exp(-gate))) * up).astype(BF16)
        h = n // 2
        away = pl.ds(pl.multiple_of(row0 + other * h, 16), h)
        cps = []
        for k, (c0, cn) in enumerate(OUT_BLOCKS):
            part[l, row0:row0 + n, c0:c0 + cn] = mm(ub[0:n], vd[l, :, c0:c0 + cn])
            cols = pl.ds(c0, cn)
            cps.append(remote(part.at[l, away, cols], prcv.at[l, pl.ds(row0 // 2, h), cols], y_peer))
            if k < now:
                send(cps[-1])
        return cps

    def home_rows(chunk):
        row0, n = chunk
        return pl.ds(pl.multiple_of(row0 + side * (n // 2), 16), n // 2)

    def home_sum(l, chunk):
        row0, n = chunk
        rows = home_rows(chunk)
        total = part[l, rows] + prcv[l, row0 // 2:row0 // 2 + n // 2]
        return (xm[rows].astype(F32) + total).astype(BF16)

    def close_layer0(chunk):
        rows = home_rows(chunk)
        x1[rows] = home_sum(0, chunk)
        return send(remote(x1.at[rows], x1.at[rows], y_peer))

    def close_layer1(chunk):
        rows = home_rows(chunk)
        hb[rows] = rms(home_sum(1, chunk).astype(F32), vfn[...].reshape(1, GAIN_PAD)[:, 0:D])
        return send(remote(hb.at[rows], hb.at[rows], y_peer))

    def head(k, rows, want_rows, n):
        hidden = hb[rows]
        ids0 = side * VOC + lax.broadcasted_iota(jnp.int32, (1, 512), 1)
        wanted = want[want_rows][:, 0:1]
        tops, sums, picked = [], [], None
        for b in range(4):
            lg = mm(hidden, vh[:, 512 * b:512 * (b + 1)])
            tops.append(jnp.max(lg, axis=-1, keepdims=True))
            sums.append(jnp.sum(jnp.exp(lg - tops[-1]), axis=-1, keepdims=True))
            hit = jnp.sum(jnp.where(ids0 + 512 * b == wanted, lg, 0.0), axis=-1, keepdims=True)
            picked = hit if picked is None else picked + hit
        top = functools.reduce(jnp.maximum, tops)
        total = sum(t * jnp.exp(m - top) for t, m in zip(sums, tops))
        table = jnp.where(lane == 0, top, jnp.where(lane == 1, total, picked))
        st_s[k, :, 0:n] = table.T[0:8]
        return send(remote(st_s.at[k], st_r.at[k], y_peer))

    def chunk_head(k, chunk):
        row0, n = chunk
        return head(k, pl.ds(row0, n), pl.ds(row0 - PIECE, n), n)

    def half_head(chunk, half):
        row0, n = chunk
        h = n // 2
        return head(2 + half, pl.ds(pl.multiple_of(row0 + half * h, 16), h), pl.ds(pl.multiple_of(row0 - PIECE + half * h, 16), h), h)

    def finish(k, t0, n):
        a, b = st_s[k, :, 0:n], st_r[k, :, 0:n]
        top = jnp.maximum(a[0:1], b[0:1])
        total = a[1:2] * jnp.exp(a[0:1] - top) + b[1:2] * jnp.exp(b[0:1] - top)
        out[0:1, t0:t0 + n] = (a[2:3] + b[2:3]) - (top + jnp.log(total))

    scope = jax.named_scope

    def wait(*cps):
        for cp in cps:
            cp.wait_recv()

    with scope('proj_p'):
        project(0, 0, PIECE, rms(vx[0:PIECE].astype(F32), van[0:1, 0:D]), PIECE)
        kv_cps = share_kv(0)
    with scope('wait_x'):
        for cp in second:
            cp.wait()
        w_my0 = [load(wo.at[0], womy.at[0, pl.ds(0, QROWS)]), load(mn, vmn.at[:, pl.ds(0, D)])]
        w_mlp0 = halves(wg, vg, 0, D) + halves(wu, vu, 0, D) + halves(wd, vd, 0, FF)
    with scope('proj_r'):
        project(0, PIECE, RESP, rms(vx[PIECE:ROWS].astype(F32), van[0:1, 0:D]), 0)
    w_qkv1 = load_qkv(1)
    w_my1 = [load(wo.at[1], womy.at[1, pl.ds(0, QROWS)])]
    w_head = [load(wh.at[pl.ds(0, D // 2)], vh.at[pl.ds(0, D // 2)]), load(wh.at[pl.ds(D // 2, D // 2)], vh.at[pl.ds(D // 2, D // 2)]),
              load(tgt, vtgt), load(fn, vfn.at[pl.ds(0, D)])]
    w_mlp1 = halves(wg, vg, 1, D) + halves(wu, vu, 1, D) + halves(wd, vd, 1, FF)
    with scope('wait_kv0'):
        wait(*kv_cps)
        expand(0, 0, kv[0])
    own = []
    with scope('relay0_0'):
        own.append(wo_relay_own(0, 0, wo_y0[0]))
    with scope('att0_p'):
        a_p = attend(0, C_P, my_pos, 0, PROMPT)
    with scope('att0_1'):
        a_1 = attend(0, C_1, 256, 256, 384)
    with scope('relay0_1'):
        own.append(wo_relay_own(0, 1, wo_y0[1]))
    with scope('att0_2'):
        a_2 = attend(0, C_2, 320, 256, 512)
    with scope('relay0_2'):
        own.append(wo_relay_own(0, 2, wo_y0[2]))
    with scope('att0_3'):
        a_3 = attend(0, C_3, 448, 384, 512)
    with scope('relay0_3'):
        own.append(wo_relay_own(0, 3, wo_y0[3]))
        wo_y1 = wo_over_y(1)
    with scope('relay0_x0'):
        dd = [wo_relay_x(0, 0, own[0][0])]
    with scope('own0'):
        for cp in w_my0:
            cp.wait()
        for ch in (C_A, C_2, C_3):
            merge_own(0, ch)
    with scope('turn_w'):
        for cp in w_qkv1:
            cp.wait()
        for j in range(5):
            wt1[:, 128 * j:128 * (j + 1)] = wqkv[1, 128 * j:128 * (j + 1)].astype(F32).T.astype(BF16)
    with scope('relay0_x123'):
        dd += [wo_relay_x(0, k, own[k][0]) for k in range(1, 4)]
    with scope('wait_w0'):
        for cp in w_mlp0 + w_head:
            cp.wait()
        for t in range(2):
            want[128 * t:128 * (t + 1)] = jnp.broadcast_to(vtgt[0:1, 128 * t:128 * (t + 1)].astype(F32), (128, 128)).T.astype(jnp.int32)
    with scope('wait_wo0'):
        wait(*[o[1] for o in own], *dd)

    with scope('wait_a0_a'):
        wait(a_p, a_1)
    with scope('merge0_a'):
        merge_attention(0, C_A, vx, (C_P, C_1))
    with scope('mlp0_a'):
        p_a = mlp(0, C_A)
    with scope('wait_a0_2'):
        wait(a_2)
    with scope('merge0_2'):
        merge_attention(0, C_2, vx, (C_2,))
    with scope('mlp0_2'):
        p_2 = mlp(0, C_2, 1)
    with scope('wait_a0_3'):
        wait(a_3)
    with scope('merge0_3'):
        merge_attention(0, C_3, vx, (C_3,))
    with scope('mlp0_3'):
        p_3 = mlp(0, C_3, 0)
    with scope('relay1'):
        own = [wo_relay_own(1, k, wo_y1[k]) for k in range(4)]
    with scope('wait_p0_a'):
        wait(*p_a)
    with scope('close0_a'):
        x_a = close_layer0(C_A)
        for cp in (p_2[1], *p_3):
            send(cp)
    with scope('relay1_x'):
        dd = [wo_relay_x(1, k, own[k][0]) for k in range(4)]
    with scope('wait_p0_2'):
        wait(*p_2)
    with scope('close0_2'):
        x_2 = close_layer0(C_2)
    with scope('wait_x_a'):
        wait(x_a)
    with scope('proj1_a'):
        project(1, 0, 128, rms(x1[0:128].astype(F32), van[1:2, 0:D]), PIECE)
        kv_cps = share_kv(1)
    with scope('wait_p0_3'):
        wait(*p_3)
    with scope('close0_3'):
        x_3 = close_layer0(C_3)

    with scope('wait_kv1'):
        wait(*kv_cps)
        for cp in w_my1:
            cp.wait()
    with scope('att1_1'):
        expand(1, 0, kv[1])
        a_1 = attend(1, C_1, 256, 256, 384)
        merge_own(1, C_1)
    with scope('wait_x_2'):
        wait(x_2)
    with scope('proj1_2'):
        project(1, 128, 128, rms(x1[128:256].astype(F32), van[1:2, 0:D]), 0)
    with scope('att1_2'):
        a_2 = attend(1, C_2, 320, 256, 512)
    with scope('wait_x_3'):
        wait(x_3)
    with scope('proj1_3'):
        project(1, 256, 64, rms(x1[256:320].astype(F32), van[1:2, 0:D]), 0)
    with scope('att1_3'):
        a_3 = attend(1, C_3, 448, 384, 512)
        merge_own(1, C_2)
    with scope('wait_w1'):
        for cp in w_mlp1:
            cp.wait()
        wait(*[o[1] for o in own], *dd)
    with scope('wait_a1_1'):
        wait(a_1)
    with scope('merge1_1'):
        merge_attention(1, C_1, x1, (C_1,))
    with scope('mlp1_1'):
        p_1 = mlp(1, C_1)
    with scope('own1_3'):
        merge_own(1, C_3)
    with scope('wait_a1_2'):
        wait(a_2)
    with scope('merge1_2'):
        merge_attention(1, C_2, x1, (C_2,))
    with scope('mlp1_2'):
        p_2 = mlp(1, C_2)
    with scope('wait_a1_3'):
        wait(a_3)
    with scope('merge1_3'):
        merge_attention(1, C_3, x1, (C_3,))
    with scope('mlp1_3'):
        p_3 = mlp(1, C_3, 0)
    with scope('wait_p1_1'):
        wait(*p_1)
    with scope('close1_1'):
        h_1 = close_layer1(C_1)
        for cp in p_3:
            send(cp)
    with scope('wait_p1_2'):
        wait(*p_2)
    with scope('close1_2'):
        h_2 = close_layer1(C_2)
    with scope('wait_h_1'):
        wait(h_1)
    with scope('head_1'):
        s_1 = chunk_head(0, C_1)
    with scope('wait_p1_3'):
        wait(*p_3)
    with scope('close1_3'):
        h_3 = close_layer1(C_3)
    with scope('head_3a'):
        s_3a = half_head(C_3, side)
    with scope('wait_h_2'):
        wait(h_2)
    with scope('head_2'):
        s_2 = chunk_head(1, C_2)
    with scope('wait_h_3'):
        wait(h_3)
    with scope('head_3'):
        s_3b = half_head(C_3, other)
    with scope('wait_s'):
        wait(s_1, s_2, s_3a, s_3b)
    with scope('finish'):
        for k, t0, n in ((0, 0, 64), (1, 64, 128), (2, 192, 32), (3, 224, 32)):
            finish(k, t0, n)
    with scope('wait_sends'):
        for cp in sent:
            cp.wait_send()


def solution(mesh):
    rows_spec = P(('prompts', 'resp'), None)
    in_specs = (rows_spec, P(('prompts', 'resp'), None, None), rows_spec, P(), P(),
                P(None, None, 'model', None), P(None, None, 'model', None), P(None, None, 'model', None),
                P(None, 'model', None, None), P(None, None, 'model'), P(None, None, 'model'),
                P(None, 'model', None), P(), P(None, 'model'))
    cos, sin = rope_constants()

    def local_pass(x_piece, x_own, tgt_own, attn_norm, mlp_norm, w_q, w_k, w_v, w_o, w_gate, w_up, w_down, final_norm, w_head):
        def rows_first(w):
            return jnp.transpose(w, (0, 2, 3, 1)).reshape(2, w.shape[2] * HD, D)

        any_spec = pl.BlockSpec(memory_space=pl.ANY)
        scratch = [
            pltpu.VMEM((ROWS, D), BF16), pltpu.VMEM((ROWS, 128), F32), pltpu.VMEM((ROWS, 128), F32), pltpu.VMEM((1, RESP), jnp.int32),
            pltpu.VMEM((2, GAIN_PAD), F32), pltpu.VMEM((2, GAIN_PAD), F32), pltpu.VMEM((GAIN_PAD,), F32),
            pltpu.VMEM((2, 640, D), BF16), pltpu.VMEM((2, 512, D), BF16), pltpu.VMEM((2, 512, D), BF16),
            pltpu.VMEM((2, D, FF), BF16), pltpu.VMEM((2, D, FF), BF16), pltpu.VMEM((2, FF, D), BF16), pltpu.VMEM((D, VOC), BF16),
            pltpu.VMEM((2, PROMPT, 128), BF16), pltpu.VMEM((2, 4, PROMPT + RESP, 128), BF16), pltpu.VMEM((D, 640), BF16), pltpu.VMEM((RESP, 128), jnp.int32),
            pltpu.VMEM((ROWS, 512), BF16), pltpu.VMEM((ROWS, 512), BF16), pltpu.VMEM((ROWS, D), F32),
            pltpu.VMEM((2, ROWS * 7 // 2, 128), BF16), pltpu.VMEM((2, ROWS * 7 // 2, 128), BF16),
            pltpu.VMEM((ROWS, D), BF16), pltpu.VMEM((128, FF), BF16),
            pltpu.VMEM((2, ROWS, D), F32), pltpu.VMEM((2, ROWS // 2, D), F32),
            pltpu.VMEM((ROWS, D), BF16), pltpu.VMEM((ROWS, D), BF16),
            pltpu.VMEM((4, 8, 128), F32), pltpu.VMEM((4, 8, 128), F32),
            pltpu.SemaphoreType.DMA((48,)), pltpu.SemaphoreType.DMA((80,)), pltpu.SemaphoreType.DMA((80,)),
        ]
        return pl.pallas_call(
            kernel,
            out_shape=jax.ShapeDtypeStruct((1, RESP), F32),
            in_specs=[any_spec] * 16,
            out_specs=pl.BlockSpec(memory_space=pltpu.VMEM),
            scratch_shapes=scratch,
            compiler_params=pltpu.CompilerParams(collective_id=0, has_side_effects=True, vmem_limit_bytes=67043328),
        )(x_piece, x_own[0], tgt_own, attn_norm, mlp_norm, rows_first(w_q), rows_first(w_k), rows_first(w_v),
          w_o.reshape(2, QROWS, D), w_gate, w_up, w_down, final_norm, w_head, jnp.asarray(cos), jnp.asarray(sin))

    return jax.shard_map(local_pass, mesh=mesh, in_specs=in_specs, out_specs=rows_spec, check_vma=False)
```

```python
import functools
import math

import jax
import jax.numpy as jnp
import numpy as np
from jax import lax
from jax.experimental import pallas as pl
from jax.experimental.pallas import tpu as pltpu
from jax.sharding import PartitionSpec as P

RMS_EPS = 1e-6
ROPE_BASE = 10000.0
NEG_BIG = -1e30
BF16 = jnp.bfloat16
F32 = jnp.float32

D = 896
HD = 64
PIECE = 64
RESP = 256
PROMPT = 256
ROWS = PIECE + RESP
FF = 2432
VOC = 2048
QROWS = 448
GROUP = 4
GAIN_PAD = 1024
C_P, C_1, C_2, C_3 = (0, 64), (64, 64), (128, 128), (256, 64)
C_A = (0, 128)
WO_QUARTER = QROWS // GROUP
WO_PIECES = (((0, 32), (32, 32), (64, 48)), ((0, 112),))
Y_WO0, Y_A, Y_WO1, Y_P, X_WO, D_WO, R_KV = (0, 1, 2), (3, 4, 5, 6), 7, (8, 9, 10), ((11, 12, 13), (14,)), (15, 16), (17, 18)
Y_SENDS, OTHER_SENDS = 8, 9
HEAD_BLOCK = 1024
FF_BLOCKS = ((0, 512), (512, 512), (1024, 512), (1536, 512), (2048, 384))


def rope_constants():
    inv = np.exp(np.arange(0, HD, 2, dtype=np.float32) * np.float32(-math.log(ROPE_BASE) / HD)).astype(np.float32)
    ang = np.arange(PROMPT + RESP, dtype=np.float32)[:, None] * inv[None, :]
    cos, sin = np.cos(ang).astype(np.float32), np.sin(ang).astype(np.float32)
    return np.concatenate([cos] * 4 + [-sin, sin] * 2, axis=1)


def mm(a, b):
    return jnp.dot(a, b, preferred_element_type=F32)


def mm_t(a, b):
    return lax.dot_general(a, b, (((1,), (1,)), ((), ())), preferred_element_type=F32)


def rms(x_f, gain):
    mean_sq = jnp.mean(x_f * x_f, axis=-1, keepdims=True)
    return (x_f * lax.rsqrt(mean_sq + RMS_EPS) * gain).astype(BF16)


def kernel(xp, xr, tgt, an, mn, wq, wk, wv, wo, wg, wu, wd, fn, wh, cs, out,
           vx, vcs, vtgt, van, vmn, vfn, wqkv, womy, woot, vg, vu, vd, vh,
           kv, kx, wt1, want, qb, amine, mo, asnd, arcv, xm, ub, part, prcv, x1, hb, st_s, st_r,
           lsem, ssem, rsem):
    me = lax.axis_index('resp')
    side = lax.axis_index('model')
    other = 1 - side
    y_peer = {'model': other}
    d_peer = {'resp': me + 1 - 2 * lax.rem(me, 2)}
    x_peer = {'resp': lax.rem(me + 2, 4)}

    def load(src, dst, k):
        cp = pltpu.make_async_copy(src, dst, lsem.at[k])
        cp.start()
        return cp

    slots = {0: [None] * Y_SENDS, 1: [None] * OTHER_SENDS}
    made = {0: 0, 1: 0}

    def remote(src, dst, peer, recv):
        pool = 0 if peer is y_peer else 1
        k = made[pool] % len(slots[pool])
        made[pool] += 1
        if slots[pool][k] is not None:
            slots[pool][k].wait_send()
        cp = pltpu.make_async_remote_copy(src_ref=src, dst_ref=dst, send_sem=ssem.at[k + pool * Y_SENDS], recv_sem=rsem.at[recv],
                                          device_id=peer, device_id_type=pl.DeviceIdType.MESH)
        slots[pool][k] = cp
        return cp

    def send(cp):
        cp.start()
        return cp

    def load_qkv(l, k):
        for src, row, n in ((wq, 0, QROWS), (wk, QROWS, HD), (wv, QROWS + HD, HD), (wv, QROWS + 2 * HD, HD)):
            load(src.at[l], wqkv.at[l, pl.ds(row, n)], k)
        return pltpu.make_async_copy(wg.at[l, pl.ds(0, 640), pl.ds(0, D)], wqkv.at[l], lsem.at[k])

    my_pos = pl.multiple_of(me * PIECE, PIECE)
    first = [load(xp, vx.at[pl.ds(0, PIECE)], 0), load(an, van.at[:, pl.ds(0, D)], 1), load_qkv(0, 2),
             load(cs.at[pl.ds(my_pos, PIECE)], vcs.at[pl.ds(0, PIECE)], 3)]
    second = [load(xr, vx.at[pl.ds(PIECE, RESP)], 4), load(cs.at[pl.ds(PROMPT, RESP)], vcs.at[pl.ds(PIECE, RESP)], 5)]

    barrier = pltpu.get_barrier_semaphore()
    pl.semaphore_signal(barrier, inc=1, device_id=y_peer, device_id_type=pl.DeviceIdType.MESH)
    for k in range(1, GROUP):
        pl.semaphore_signal(barrier, inc=1, device_id={'resp': lax.rem(me + k, GROUP)}, device_id_type=pl.DeviceIdType.MESH)
    pl.semaphore_wait(barrier, GROUP)

    def wo_slot(l, q, piece):
        start, size = WO_PIECES[l][piece]
        return pl.ds(pl.multiple_of(q * WO_QUARTER + start, 16), size)

    def wo_over_y(l, recvs):
        cps = []
        for k, recv in enumerate(recvs):
            rows = wo_slot(l, me, k)
            cps.append(send(remote(wo.at[l, rows], woot.at[l, rows], y_peer, recv)))
        return cps

    def wo_relay(l, piece, quarter, copy, to_x):
        copy.wait_recv()
        slot = woot.at[l, wo_slot(l, quarter, piece)]
        over_x = send(remote(slot, slot, x_peer, X_WO[l][piece])) if to_x else None
        send(remote(slot, slot, d_peer, D_WO[l]))
        return over_x

    def wo_relay_own(l, piece, copy):
        return wo_relay(l, piece, me, copy, True)

    def wo_relay_x(l, piece, copy):
        return wo_relay(l, piece, lax.rem(me + 2, 4), copy, False)

    def wait_wo_core(l):
        both = woot.at[l, pl.ds(0, 2 * WO_QUARTER)]
        pltpu.make_async_remote_copy(src_ref=both, dst_ref=both, send_sem=ssem.at[0], recv_sem=rsem.at[D_WO[l]],
                                     device_id=d_peer, device_id_type=pl.DeviceIdType.MESH).wait_recv()

    wo_y0 = wo_over_y(0, Y_WO0)

    zeros = jnp.zeros((512 - QROWS, D), BF16)
    for l in range(2):
        womy[l, QROWS:512] = zeros
        woot[l, QROWS:512] = zeros
    for k in range(4):
        kx[1, k, PROMPT:PROMPT + RESP] = jnp.zeros((RESP, 128), BF16)

    for cp in first:
        cp.wait()

    lane = lax.broadcasted_iota(jnp.int32, (1, 128), 1)
    lo_head = lane < HD
    lo_half = lax.rem(lane, HD) < (HD // 2)

    def expand(l, row0, pair):
        f = pair.astype(F32)
        r = pltpu.roll(f, HD, 1)
        n = pair.shape[0]
        kx[l, 0, row0:row0 + n] = jnp.where(lo_head, r, 0.0).astype(BF16)
        kx[l, 1, row0:row0 + n] = jnp.where(lo_head, 0.0, f).astype(BF16)
        kx[l, 2, row0:row0 + n] = jnp.where(lo_head, f, 0.0).astype(BF16)
        kx[l, 3, row0:row0 + n] = jnp.where(lo_head, 0.0, r).astype(BF16)

    def project(l, row0, n, hidden, piece_rows):
        y = mm(hidden, wt1[...]) if l else mm_t(hidden, wqkv[l])
        cos, sin = vcs[row0:row0 + n, 0:128], vcs[row0:row0 + n, 128:256]
        roped = []
        for j in range(4):
            b = y[:, 128 * j:128 * (j + 1)]
            partner = jnp.where(lo_half, pltpu.roll(b, 128 - HD // 2, 1), pltpu.roll(b, HD // 2, 1))
            roped.append(b * cos + partner * sin)
            qb[row0:row0 + n, 128 * j:128 * (j + 1)] = roped[-1].astype(BF16)
        pair = jnp.where(lo_head, y[:, 512:640], roped[3]).astype(BF16)
        if piece_rows:
            kv[l, pl.ds(my_pos, PIECE)] = pair[0:PIECE]
        if n > piece_rows:
            expand(l, PROMPT + row0 + piece_rows - PIECE, pair[piece_rows:n])

    def share_kv(l):
        slot = kv.at[l, pl.ds(my_pos, PIECE)]
        for k in range(1, GROUP):
            send(remote(slot, slot, {'resp': lax.rem(me + k, GROUP)}, R_KV[l]))
        three = kv.at[l, pl.ds(0, 3 * PIECE)]
        return pltpu.make_async_remote_copy(src_ref=three, dst_ref=three, send_sem=ssem.at[0], recv_sem=rsem.at[R_KV[l]],
                                            device_id=d_peer, device_id_type=pl.DeviceIdType.MESH)

    def a_base(row0):
        return row0 * 7 // 2

    def attend(l, chunk, base, vis, nk, recv):
        row0, n = chunk
        k_even, k_odd, v_even, v_odd = (kx[l, k, 0:nk] for k in range(4))
        q = [qb[row0:row0 + n, 128 * j:128 * (j + 1)] for j in range(4)]
        s_even = mm_t(jnp.concatenate(q, axis=0), k_even)
        s_odd = mm_t(jnp.concatenate(q[:3], axis=0), k_odd)
        keep = (lax.broadcasted_iota(jnp.int32, (n, nk - vis), 1) + vis) <= (base + lax.broadcasted_iota(jnp.int32, (n, nk - vis), 0))

        def probs(s):
            tail = jnp.where(keep, s[:, vis:], NEG_BIG)
            s = jnp.concatenate([s[:, :vis], tail], axis=1) if vis else tail
            top = jnp.max(s, axis=-1, keepdims=True)
            e = jnp.exp2((s - top) * (math.log2(math.e) / math.sqrt(HD)))
            return (e * (1.0 / jnp.sum(e, axis=-1, keepdims=True))).astype(BF16)

        p_even = jnp.concatenate([probs(s_even[j * n:(j + 1) * n]) for j in range(4)], axis=0)
        p_odd = jnp.concatenate([probs(s_odd[j * n:(j + 1) * n]) for j in range(3)], axis=0)
        o_even = mm(p_even, v_even)
        o_odd = mm(p_odd, v_odd)
        ab = a_base(row0)
        for j in range(3):
            blk = (o_even[j * n:(j + 1) * n] + o_odd[j * n:(j + 1) * n]).astype(BF16)
            amine[row0:row0 + n, 128 * j:128 * (j + 1)] = blk
            asnd[l, ab + j * n:ab + (j + 1) * n] = blk
        last = o_even[3 * n:4 * n]
        amine[row0:row0 + n, 384:512] = last.astype(BF16)
        asnd[l, ab + 3 * n:ab + 7 * n // 2] = (last[:n // 2] + pltpu.roll(last[n // 2:], HD, 1)).astype(BF16)
        rows = pl.ds(ab, 7 * n // 2)
        return send(remote(asnd.at[l, rows], arcv.at[l, rows], y_peer, recv))

    def merge_own(l, chunk):
        row0, n = chunk
        mo[row0:row0 + n] = mm(amine[row0:row0 + n], womy[l])

    def received(l, chunk):
        row0, n = chunk
        ab = a_base(row0)
        packed = arcv[l, ab + 3 * n:ab + 7 * n // 2].astype(F32)
        last = jnp.concatenate([packed, pltpu.roll(packed, HD, 1)], axis=0).astype(BF16)
        return jnp.concatenate([arcv[l, ab + j * n:ab + (j + 1) * n] for j in range(3)] + [last], axis=1)

    def merge_attention(l, chunk, x_ref, parts):
        row0, n = chunk
        a_oth = jnp.concatenate([received(l, p) for p in parts], axis=0)
        proj = mo[row0:row0 + n] + mm(a_oth, woot[l])
        xm[row0:row0 + n] = (x_ref[row0:row0 + n].astype(F32) + proj).astype(BF16)

    def mlp(l, chunk, recv):
        row0, n = chunk
        g = rms(xm[row0:row0 + n].astype(F32), vmn[l:l + 1, 0:D])
        for b0, bn in FF_BLOCKS:
            gate = mm(g, vg[l, :, b0:b0 + bn])
            up = mm(g, vu[l, :, b0:b0 + bn])
            ub[0:n, b0:b0 + bn] = (gate * (1.0 / (1.0 + jnp.exp(-gate))) * up).astype(BF16)
        part[l, row0:row0 + n] = mm(ub[0:n], vd[l])
        h = n // 2
        away = pl.ds(pl.multiple_of(row0 + other * h, 16), h)
        return remote(part.at[l, away], prcv.at[l, pl.ds(row0 // 2, h)], y_peer, recv)

    def home_rows(chunk):
        row0, n = chunk
        return pl.ds(pl.multiple_of(row0 + side * (n // 2), 16), n // 2)

    def home_sum(l, chunk):
        row0, n = chunk
        rows = home_rows(chunk)
        total = part[l, rows] + prcv[l, row0 // 2:row0 // 2 + n // 2]
        return (xm[rows].astype(F32) + total).astype(BF16)

    def close_layer0(chunk, recv):
        rows = home_rows(chunk)
        x1[rows] = home_sum(0, chunk)
        return send(remote(x1.at[rows], x1.at[rows], y_peer, recv))

    def close_layer1(chunk, recv):
        rows = home_rows(chunk)
        hb[rows] = rms(home_sum(1, chunk).astype(F32), vfn[...].reshape(1, GAIN_PAD)[:, 0:D])
        return send(remote(hb.at[rows], hb.at[rows], y_peer, recv))

    def head(k, chunk, recv):
        row0, n = chunk
        hidden = hb[row0:row0 + n]
        ids0 = side * VOC + lax.broadcasted_iota(jnp.int32, (1, HEAD_BLOCK), 1)
        wanted = want[row0 - PIECE:row0 - PIECE + n, 0:1]
        tops, sums, picked = [], [], None
        for b in range(VOC // HEAD_BLOCK):
            lg = mm(hidden, vh[:, HEAD_BLOCK * b:HEAD_BLOCK * (b + 1)])
            tops.append(jnp.max(lg, axis=-1, keepdims=True))
            sums.append(jnp.sum(jnp.exp(lg - tops[-1]), axis=-1, keepdims=True))
            hit = jnp.sum(jnp.where(ids0 + HEAD_BLOCK * b == wanted, lg, 0.0), axis=-1, keepdims=True)
            picked = hit if picked is None else picked + hit
        top = functools.reduce(jnp.maximum, tops)
        total = sum(t * jnp.exp(m - top) for t, m in zip(sums, tops))
        table = jnp.where(lane == 0, top, jnp.where(lane == 1, total, picked))
        st_s[k, :, 0:n] = table.T[0:8]
        return send(remote(st_s.at[k], st_r.at[k], y_peer, recv))

    def finish(k, t0, n):
        a, b = st_s[k, :, 0:n], st_r[k, :, 0:n]
        top = jnp.maximum(a[0:1], b[0:1])
        total = a[1:2] * jnp.exp(a[0:1] - top) + b[1:2] * jnp.exp(b[0:1] - top)
        out[0:1, t0:t0 + n] = (a[2:3] + b[2:3]) - (top + jnp.log(total))

    scope = jax.named_scope

    def wait(*cps):
        for cp in cps:
            cp.wait_recv()

    with scope('proj_p'):
        project(0, 0, PIECE, rms(vx[0:PIECE].astype(F32), van[0:1, 0:D]), PIECE)
        kv_cps = share_kv(0)
    with scope('wait_x'):
        for cp in second:
            cp.wait()
        w_my0 = [load(wo.at[0], womy.at[0, pl.ds(0, QROWS)], 6), load(mn, vmn.at[:, pl.ds(0, D)], 7)]
        w_mlp0 = [load(wg.at[0], vg.at[0], 8), load(wu.at[0], vu.at[0], 9), load(wd.at[0], vd.at[0], 10)]
    with scope('proj_r'):
        project(0, PIECE, RESP, rms(vx[PIECE:ROWS].astype(F32), van[0:1, 0:D]), 0)
    w_qkv1 = load_qkv(1, 2)
    w_my1 = load(wo.at[1], womy.at[1, pl.ds(0, QROWS)], 0)
    w_head = [load(wh, vh, 3), load(tgt, vtgt, 4), load(fn, vfn.at[pl.ds(0, D)], 5)]
    with scope('wait_kv0'):
        wait(kv_cps)
        expand(0, 0, kv[0])
    own = []
    with scope('relay0_0'):
        own.append(wo_relay_own(0, 0, wo_y0[0]))
    with scope('att0_p'):
        a_p = attend(0, C_P, my_pos, 0, PROMPT, Y_A[0])
    with scope('att0_1'):
        a_1 = attend(0, C_1, 256, 256, 384, Y_A[1])
    with scope('relay0_1'):
        own.append(wo_relay_own(0, 1, wo_y0[1]))
    with scope('att0_2'):
        a_2 = attend(0, C_2, 320, 256, 512, Y_A[2])
    with scope('relay0_2'):
        own.append(wo_relay_own(0, 2, wo_y0[2]))
    with scope('att0_3'):
        a_3 = attend(0, C_3, 448, 384, 512, Y_A[3])
    with scope('wo1'):
        wo_y1 = wo_over_y(1, (Y_WO1,))
    with scope('relay0_x0'):
        wo_relay_x(0, 0, own[0])
    with scope('own0'):
        for cp in w_my0:
            cp.wait()
        for ch in (C_A, C_2, C_3):
            merge_own(0, ch)
    with scope('turn_w'):
        w_qkv1.wait()
        for j in range(5):
            wt1[:, 128 * j:128 * (j + 1)] = wqkv[1, 128 * j:128 * (j + 1)].astype(F32).T.astype(BF16)
    with scope('relay0_x123'):
        for k in range(1, 3):
            wo_relay_x(0, k, own[k])
    with scope('wait_w0'):
        for cp in w_mlp0 + w_head:
            cp.wait()
        w_mlp1 = [load(wg.at[1], vg.at[1], 8), load(wu.at[1], vu.at[1], 9), load(wd.at[1], vd.at[1], 10)]
        for t in range(2):
            want[128 * t:128 * (t + 1)] = jnp.broadcast_to(vtgt[0:1, 128 * t:128 * (t + 1)].astype(F32), (128, 128)).T.astype(jnp.int32)
    with scope('wait_wo0'):
        wait_wo_core(0)

    with scope('wait_a0_a'):
        wait(a_p, a_1)
    with scope('merge0_a'):
        merge_attention(0, C_A, vx, (C_P, C_1))
    with scope('mlp0_a'):
        p_a = send(mlp(0, C_A, Y_P[0]))
    with scope('wait_a0_2'):
        wait(a_2)
    with scope('merge0_2'):
        merge_attention(0, C_2, vx, (C_2,))
    with scope('mlp0_2'):
        p_2 = send(mlp(0, C_2, Y_P[1]))
    with scope('wait_a0_3'):
        wait(a_3)
    with scope('merge0_3'):
        merge_attention(0, C_3, vx, (C_3,))
    with scope('mlp0_3'):
        p_3 = mlp(0, C_3, Y_P[2])
    with scope('relay1'):
        own1 = wo_relay_own(1, 0, wo_y1[0])
    with scope('wait_p0_a'):
        wait(p_a)
    with scope('close0_a'):
        x_a = close_layer0(C_A, Y_WO0[0])
        send(p_3)
    with scope('relay1_x'):
        wo_relay_x(1, 0, own1)
    with scope('wait_p0_2'):
        wait(p_2)
    with scope('close0_2'):
        x_2 = close_layer0(C_2, Y_WO0[1])
    with scope('wait_x_a'):
        wait(x_a)
    with scope('proj1_a'):
        project(1, 0, 128, rms(x1[0:128].astype(F32), van[1:2, 0:D]), PIECE)
        kv_cps = share_kv(1)
    with scope('wait_p0_3'):
        wait(p_3)
    with scope('close0_3'):
        x_3 = close_layer0(C_3, Y_WO0[2])

    with scope('wait_kv1'):
        wait(kv_cps)
        w_my1.wait()
    with scope('att1_1'):
        expand(1, 0, kv[1])
        a_1 = attend(1, C_1, 256, 256, 384, Y_A[1])
        merge_own(1, C_1)
    with scope('wait_x_2'):
        wait(x_2)
    with scope('proj1_2'):
        project(1, 128, 128, rms(x1[128:256].astype(F32), van[1:2, 0:D]), 0)
    with scope('att1_2'):
        a_2 = attend(1, C_2, 320, 256, 512, Y_A[2])
    with scope('wait_x_3'):
        wait(x_3)
    with scope('proj1_3'):
        project(1, 256, 64, rms(x1[256:320].astype(F32), van[1:2, 0:D]), 0)
    with scope('att1_3'):
        a_3 = attend(1, C_3, 448, 384, 512, Y_A[3])
        merge_own(1, C_2)
    with scope('wait_w1'):
        for cp in w_mlp1:
            cp.wait()
        wait_wo_core(1)
    with scope('wait_a1_1'):
        wait(a_1)
    with scope('merge1_1'):
        merge_attention(1, C_1, x1, (C_1,))
    with scope('mlp1_1'):
        p_1 = send(mlp(1, C_1, Y_P[0]))
    with scope('own1_3'):
        merge_own(1, C_3)
    with scope('wait_a1_2'):
        wait(a_2)
    with scope('merge1_2'):
        merge_attention(1, C_2, x1, (C_2,))
    with scope('mlp1_2'):
        p_2 = send(mlp(1, C_2, Y_P[1]))
    with scope('wait_a1_3'):
        wait(a_3)
    with scope('merge1_3'):
        merge_attention(1, C_3, x1, (C_3,))
    with scope('mlp1_3'):
        p_3 = mlp(1, C_3, Y_P[2])
    with scope('wait_p1_1'):
        wait(p_1)
    with scope('close1_1'):
        h_1 = close_layer1(C_1, Y_WO0[0])
        send(p_3)
    with scope('wait_p1_2'):
        wait(p_2)
    with scope('close1_2'):
        h_2 = close_layer1(C_2, Y_WO0[1])
    with scope('wait_h_1'):
        wait(h_1)
    with scope('head_1'):
        s_1 = head(0, C_1, Y_A[0])
    with scope('wait_p1_3'):
        wait(p_3)
    with scope('close1_3'):
        h_3 = close_layer1(C_3, Y_WO0[2])
    with scope('wait_h_2'):
        wait(h_2)
    with scope('head_2'):
        s_2 = head(1, C_2, Y_WO1)
    with scope('wait_h_3'):
        wait(h_3)
    with scope('head_3'):
        s_3 = head(2, C_3, Y_A[1])
    with scope('wait_s'):
        wait(s_1, s_2, s_3)
    with scope('finish'):
        for k, t0, n in ((0, 0, 64), (1, 64, 128), (2, 192, 64)):
            finish(k, t0, n)
    with scope('wait_sends'):
        for pool in slots.values():
            for cp in pool:
                cp.wait_send()


def solution(mesh):
    rows_spec = P(('prompts', 'resp'), None)
    in_specs = (rows_spec, P(('prompts', 'resp'), None, None), rows_spec, P(), P(),
                P(None, None, 'model', None), P(None, None, 'model', None), P(None, None, 'model', None),
                P(None, 'model', None, None), P(None, None, 'model'), P(None, None, 'model'),
                P(None, 'model', None), P(), P(None, 'model'))
    table = rope_constants()

    def local_pass(x_piece, x_own, tgt_own, attn_norm, mlp_norm, w_q, w_k, w_v, w_o, w_gate, w_up, w_down, final_norm, w_head):
        def rows_first(w):
            return jnp.transpose(w, (0, 2, 3, 1)).reshape(2, w.shape[2] * HD, D)

        any_spec = pl.BlockSpec(memory_space=pl.ANY)
        scratch = [
            pltpu.VMEM((ROWS, D), BF16), pltpu.VMEM((ROWS, 256), F32), pltpu.VMEM((1, RESP), jnp.int32),
            pltpu.VMEM((2, GAIN_PAD), F32), pltpu.VMEM((2, GAIN_PAD), F32), pltpu.VMEM((GAIN_PAD,), F32),
            pltpu.VMEM((2, 640, D), BF16), pltpu.VMEM((2, 512, D), BF16), pltpu.VMEM((2, 512, D), BF16),
            pltpu.VMEM((2, D, FF), BF16), pltpu.VMEM((2, D, FF), BF16), pltpu.VMEM((2, FF, D), BF16), pltpu.VMEM((D, VOC), BF16),
            pltpu.VMEM((2, PROMPT, 128), BF16), pltpu.VMEM((2, 4, PROMPT + RESP, 128), BF16), pltpu.VMEM((D, 640), BF16), pltpu.VMEM((RESP, 128), jnp.int32),
            pltpu.VMEM((ROWS, 512), BF16), pltpu.VMEM((ROWS, 512), BF16), pltpu.VMEM((ROWS, D), F32),
            pltpu.VMEM((2, ROWS * 7 // 2, 128), BF16), pltpu.VMEM((2, ROWS * 7 // 2, 128), BF16),
            pltpu.VMEM((ROWS, D), BF16), pltpu.VMEM((128, FF), BF16),
            pltpu.VMEM((2, ROWS, D), F32), pltpu.VMEM((2, ROWS // 2, D), F32),
            pltpu.VMEM((ROWS, D), BF16), pltpu.VMEM((ROWS, D), BF16),
            pltpu.VMEM((3, 8, 128), F32), pltpu.VMEM((3, 8, 128), F32),
            pltpu.SemaphoreType.DMA((11,)), pltpu.SemaphoreType.DMA((Y_SENDS + OTHER_SENDS,)), pltpu.SemaphoreType.DMA((19,)),
        ]
        return pl.pallas_call(
            kernel,
            out_shape=jax.ShapeDtypeStruct((1, RESP), F32),
            in_specs=[any_spec] * 15,
            out_specs=pl.BlockSpec(memory_space=pltpu.VMEM),
            scratch_shapes=scratch,
            compiler_params=pltpu.CompilerParams(collective_id=0, has_side_effects=True, vmem_limit_bytes=67043328),
        )(x_piece, x_own[0], tgt_own, attn_norm, mlp_norm, rows_first(w_q), rows_first(w_k), rows_first(w_v),
          w_o.reshape(2, QROWS, D), w_gate, w_up, w_down, final_norm, w_head, jnp.asarray(table))

    return jax.shard_map(local_pass, mesh=mesh, in_specs=in_specs, out_specs=rows_spec, check_vma=False)
```

```python
import functools
import math

import jax
import jax.numpy as jnp
import numpy as np
from jax import lax
from jax.experimental import pallas as pl
from jax.experimental.pallas import tpu as pltpu
from jax.sharding import PartitionSpec as P

RMS_EPS = 1e-6
ROPE_BASE = 10000.0
NEG_BIG = -1e30
BF16 = jnp.bfloat16
F32 = jnp.float32

D = 896
HD = 64
PIECE = 64
RESP = 256
PROMPT = 256
ROWS = PIECE + RESP
FF = 2432
VOC = 2048
QROWS = 448
GROUP = 4
GAIN_PAD = 1024
C_P, C_1, C_2, C_3 = (0, 64), (64, 64), (128, 128), (256, 64)
C_A = (0, 128)
WO_QUARTER = QROWS // GROUP
WO_PIECES = (((0, 32), (32, 32), (64, 48)), ((0, 112),))
Y_WO0, Y_A, Y_WO1, Y_P, X_WO, D_WO, R_KV = (0, 1, 2), (3, 4, 5, 6), 7, (8, 9, 10), ((11, 12, 13), (14,)), (15, 16), (17, 18)
Y_SENDS, OTHER_SENDS = 8, 9
HEAD_BLOCK = 1024
FF_BLOCKS = ((0, 512), (512, 512), (1024, 512), (1536, 512), (2048, 384))


def rope_constants():
    inv = np.exp(np.arange(0, HD, 2, dtype=np.float32) * np.float32(-math.log(ROPE_BASE) / HD)).astype(np.float32)
    ang = np.arange(PROMPT + RESP, dtype=np.float32)[:, None] * inv[None, :]
    cos, sin = np.cos(ang).astype(np.float32), np.sin(ang).astype(np.float32)
    return np.concatenate([cos] * 4 + [-sin, sin] * 2, axis=1)


def mm(a, b):
    return jnp.dot(a, b, preferred_element_type=F32)


def mm_t(a, b):
    return lax.dot_general(a, b, (((1,), (1,)), ((), ())), preferred_element_type=F32)


def rms(x_f, gain):
    mean_sq = jnp.mean(x_f * x_f, axis=-1, keepdims=True)
    return (x_f * lax.rsqrt(mean_sq + RMS_EPS) * gain).astype(BF16)


def kernel(xp, xr, tgt, an, mn, wq, wk, wv, wo, wg, wu, wd, fn, wh, cs, out,
           vx, vcs, vtgt, van, vmn, vfn, wqkv, womy, woot, vg, vu, vd, vh,
           kv, kx, wt1, want, qb, amine, mo, asnd, arcv, xm, ub, part, prcv, x1, hb, st_s, st_r,
           lsem, ssem, rsem):
    me = lax.axis_index('resp')
    side = lax.axis_index('model')
    other = 1 - side
    y_peer = {'model': other}
    d_peer = {'resp': me + 1 - 2 * lax.rem(me, 2)}
    x_peer = {'resp': lax.rem(me + 2, 4)}

    barrier = pltpu.get_barrier_semaphore()
    pl.semaphore_signal(barrier, inc=1, device_id=y_peer, device_id_type=pl.DeviceIdType.MESH)
    for k in range(1, GROUP):
        pl.semaphore_signal(barrier, inc=1, device_id={'resp': lax.rem(me + k, GROUP)}, device_id_type=pl.DeviceIdType.MESH)

    def load(src, dst, k):
        cp = pltpu.make_async_copy(src, dst, lsem.at[k])
        cp.start()
        return cp

    slots = {0: [None] * Y_SENDS, 1: [None] * OTHER_SENDS}
    made = {0: 0, 1: 0}

    def remote(src, dst, peer, recv):
        pool = 0 if peer is y_peer else 1
        k = made[pool] % len(slots[pool])
        made[pool] += 1
        if slots[pool][k] is not None:
            slots[pool][k].wait_send()
        cp = pltpu.make_async_remote_copy(src_ref=src, dst_ref=dst, send_sem=ssem.at[k + pool * Y_SENDS], recv_sem=rsem.at[recv],
                                          device_id=peer, device_id_type=pl.DeviceIdType.MESH)
        slots[pool][k] = cp
        return cp

    def send(cp):
        cp.start()
        return cp

    def load_qkv(l, k):
        for src, row, n in ((wq, 0, QROWS), (wk, QROWS, HD), (wv, QROWS + HD, HD), (wv, QROWS + 2 * HD, HD)):
            load(src.at[l], wqkv.at[l, pl.ds(row, n)], k)
        return pltpu.make_async_copy(wg.at[l, pl.ds(0, 640), pl.ds(0, D)], wqkv.at[l], lsem.at[k])

    my_pos = pl.multiple_of(me * PIECE, PIECE)
    first = [load(xp, vx.at[pl.ds(0, PIECE)], 0), load(an, van.at[:, pl.ds(0, D)], 1), load_qkv(0, 2),
             load(cs.at[pl.ds(my_pos, PIECE)], vcs.at[pl.ds(0, PIECE)], 3)]
    second = [load(xr, vx.at[pl.ds(PIECE, RESP)], 4), load(cs.at[pl.ds(PROMPT, RESP)], vcs.at[pl.ds(PIECE, RESP)], 5)]

    pl.semaphore_wait(barrier, GROUP)

    def wo_slot(l, q, piece):
        start, size = WO_PIECES[l][piece]
        return pl.ds(pl.multiple_of(q * WO_QUARTER + start, 16), size)

    def wo_over_y(l, recvs):
        cps = []
        for k, recv in enumerate(recvs):
            rows = wo_slot(l, me, k)
            cps.append(send(remote(wo.at[l, rows], woot.at[l, rows], y_peer, recv)))
        return cps

    def wo_relay(l, piece, quarter, copy, to_x):
        copy.wait_recv()
        slot = woot.at[l, wo_slot(l, quarter, piece)]
        over_x = send(remote(slot, slot, x_peer, X_WO[l][piece])) if to_x else None
        send(remote(slot, slot, d_peer, D_WO[l]))
        return over_x

    def wo_relay_own(l, piece, copy):
        return wo_relay(l, piece, me, copy, True)

    def wo_relay_x(l, piece, copy):
        return wo_relay(l, piece, lax.rem(me + 2, 4), copy, False)

    def wait_wo_core(l):
        both = woot.at[l, pl.ds(0, 2 * WO_QUARTER)]
        pltpu.make_async_remote_copy(src_ref=both, dst_ref=both, send_sem=ssem.at[0], recv_sem=rsem.at[D_WO[l]],
                                     device_id=d_peer, device_id_type=pl.DeviceIdType.MESH).wait_recv()

    wo_y0 = wo_over_y(0, Y_WO0)

    zeros = jnp.zeros((512 - QROWS, D), BF16)
    for l in range(2):
        womy[l, QROWS:512] = zeros
        woot[l, QROWS:512] = zeros
    for k in range(4):
        kx[1, k, PROMPT:PROMPT + RESP] = jnp.zeros((RESP, 128), BF16)

    for cp in first:
        cp.wait()

    lane = lax.broadcasted_iota(jnp.int32, (1, 128), 1)
    lo_head = lane < HD
    lo_half = lax.rem(lane, HD) < (HD // 2)

    def expand(l, row0, pair):
        f = pair.astype(F32)
        r = pltpu.roll(f, HD, 1)
        n = pair.shape[0]
        kx[l, 0, row0:row0 + n] = jnp.where(lo_head, r, 0.0).astype(BF16)
        kx[l, 1, row0:row0 + n] = jnp.where(lo_head, 0.0, f).astype(BF16)
        kx[l, 2, row0:row0 + n] = jnp.where(lo_head, f, 0.0).astype(BF16)
        kx[l, 3, row0:row0 + n] = jnp.where(lo_head, 0.0, r).astype(BF16)

    def project(l, row0, n, hidden, piece_rows):
        y = mm(hidden, wt1[...]) if l else mm_t(hidden, wqkv[l])
        cos, sin = vcs[row0:row0 + n, 0:128], vcs[row0:row0 + n, 128:256]
        roped = []
        for j in range(4):
            b = y[:, 128 * j:128 * (j + 1)]
            partner = jnp.where(lo_half, pltpu.roll(b, 128 - HD // 2, 1), pltpu.roll(b, HD // 2, 1))
            roped.append(b * cos + partner * sin)
            qb[row0:row0 + n, 128 * j:128 * (j + 1)] = roped[-1].astype(BF16)
        pair = jnp.where(lo_head, y[:, 512:640], roped[3]).astype(BF16)
        if piece_rows:
            kv[l, pl.ds(my_pos, PIECE)] = pair[0:PIECE]
        if n > piece_rows:
            expand(l, PROMPT + row0 + piece_rows - PIECE, pair[piece_rows:n])

    def share_kv(l):
        slot = kv.at[l, pl.ds(my_pos, PIECE)]
        for k in range(1, GROUP):
            send(remote(slot, slot, {'resp': lax.rem(me + k, GROUP)}, R_KV[l]))
        three = kv.at[l, pl.ds(0, 3 * PIECE)]
        return pltpu.make_async_remote_copy(src_ref=three, dst_ref=three, send_sem=ssem.at[0], recv_sem=rsem.at[R_KV[l]],
                                            device_id=d_peer, device_id_type=pl.DeviceIdType.MESH)

    def a_base(row0):
        return row0 * 7 // 2

    def attend(l, chunk, base, vis, nk, recv):
        row0, n = chunk
        k_even, k_odd, v_even, v_odd = (kx[l, k, 0:nk] for k in range(4))
        q = [qb[row0:row0 + n, 128 * j:128 * (j + 1)] for j in range(4)]
        s_even = mm_t(jnp.concatenate(q, axis=0), k_even)
        s_odd = mm_t(jnp.concatenate(q[:3], axis=0), k_odd)
        keep = (lax.broadcasted_iota(jnp.int32, (n, nk - vis), 1) + vis) <= (base + lax.broadcasted_iota(jnp.int32, (n, nk - vis), 0))

        def probs(s):
            tail = jnp.where(keep, s[:, vis:], NEG_BIG)
            s = jnp.concatenate([s[:, :vis], tail], axis=1) if vis else tail
            top = jnp.max(s, axis=-1, keepdims=True)
            e = jnp.exp2((s - top) * (math.log2(math.e) / math.sqrt(HD)))
            return (e * (1.0 / jnp.sum(e, axis=-1, keepdims=True))).astype(BF16)

        p_even = jnp.concatenate([probs(s_even[j * n:(j + 1) * n]) for j in range(4)], axis=0)
        p_odd = jnp.concatenate([probs(s_odd[j * n:(j + 1) * n]) for j in range(3)], axis=0)
        o_even = mm(p_even, v_even)
        o_odd = mm(p_odd, v_odd)
        ab = a_base(row0)
        for j in range(3):
            blk = (o_even[j * n:(j + 1) * n] + o_odd[j * n:(j + 1) * n]).astype(BF16)
            amine[row0:row0 + n, 128 * j:128 * (j + 1)] = blk
            asnd[l, ab + j * n:ab + (j + 1) * n] = blk
        last = o_even[3 * n:4 * n]
        amine[row0:row0 + n, 384:512] = last.astype(BF16)
        asnd[l, ab + 3 * n:ab + 7 * n // 2] = (last[:n // 2] + pltpu.roll(last[n // 2:], HD, 1)).astype(BF16)
        rows = pl.ds(ab, 7 * n // 2)
        return send(remote(asnd.at[l, rows], arcv.at[l, rows], y_peer, recv))

    def merge_own(l, chunk):
        row0, n = chunk
        mo[row0:row0 + n] = mm(amine[row0:row0 + n], womy[l])

    def received(l, chunk):
        row0, n = chunk
        ab = a_base(row0)
        packed = arcv[l, ab + 3 * n:ab + 7 * n // 2].astype(F32)
        last = jnp.concatenate([packed, pltpu.roll(packed, HD, 1)], axis=0).astype(BF16)
        return jnp.concatenate([arcv[l, ab + j * n:ab + (j + 1) * n] for j in range(3)] + [last], axis=1)

    def merge_attention(l, chunk, x_ref, parts):
        row0, n = chunk
        a_oth = jnp.concatenate([received(l, p) for p in parts], axis=0)
        proj = mo[row0:row0 + n] + mm(a_oth, woot[l])
        xm[row0:row0 + n] = (x_ref[row0:row0 + n].astype(F32) + proj).astype(BF16)

    def mlp(l, chunk, recv):
        row0, n = chunk
        g = rms(xm[row0:row0 + n].astype(F32), vmn[l:l + 1, 0:D])
        for b0, bn in FF_BLOCKS:
            gate = mm(g, vg[l, :, b0:b0 + bn])
            up = mm(g, vu[l, :, b0:b0 + bn])
            ub[0:n, b0:b0 + bn] = (gate * (1.0 / (1.0 + jnp.exp(-gate))) * up).astype(BF16)
        part[l, row0:row0 + n] = mm(ub[0:n], vd[l])
        h = n // 2
        away = pl.ds(pl.multiple_of(row0 + other * h, 16), h)
        return remote(part.at[l, away], prcv.at[l, pl.ds(row0 // 2, h)], y_peer, recv)

    def home_rows(chunk):
        row0, n = chunk
        return pl.ds(pl.multiple_of(row0 + side * (n // 2), 16), n // 2)

    def home_sum(l, chunk):
        row0, n = chunk
        rows = home_rows(chunk)
        total = part[l, rows] + prcv[l, row0 // 2:row0 // 2 + n // 2]
        return (xm[rows].astype(F32) + total).astype(BF16)

    def close_layer0(chunk, recv):
        rows = home_rows(chunk)
        x1[rows] = home_sum(0, chunk)
        return send(remote(x1.at[rows], x1.at[rows], y_peer, recv))

    def close_layer1(chunk, recv):
        rows = home_rows(chunk)
        hb[rows] = rms(home_sum(1, chunk).astype(F32), vfn[...].reshape(1, GAIN_PAD)[:, 0:D])
        return send(remote(hb.at[rows], hb.at[rows], y_peer, recv))

    def head(k, chunk, recv):
        row0, n = chunk
        hidden = hb[row0:row0 + n]
        ids0 = side * VOC + lax.broadcasted_iota(jnp.int32, (1, HEAD_BLOCK), 1)
        wanted = want[row0 - PIECE:row0 - PIECE + n, 0:1]
        tops, sums, picked = [], [], None
        for b in range(VOC // HEAD_BLOCK):
            lg = mm(hidden, vh[:, HEAD_BLOCK * b:HEAD_BLOCK * (b + 1)])
            tops.append(jnp.max(lg, axis=-1, keepdims=True))
            sums.append(jnp.sum(jnp.exp(lg - tops[-1]), axis=-1, keepdims=True))
            hit = jnp.sum(jnp.where(ids0 + HEAD_BLOCK * b == wanted, lg, 0.0), axis=-1, keepdims=True)
            picked = hit if picked is None else picked + hit
        top = functools.reduce(jnp.maximum, tops)
        total = sum(t * jnp.exp(m - top) for t, m in zip(sums, tops))
        table = jnp.where(lane == 0, top, jnp.where(lane == 1, total, picked))
        st_s[k, :, 0:n] = table.T[0:8]
        return send(remote(st_s.at[k], st_r.at[k], y_peer, recv))

    def finish(k, t0, n):
        a, b = st_s[k, :, 0:n], st_r[k, :, 0:n]
        top = jnp.maximum(a[0:1], b[0:1])
        total = a[1:2] * jnp.exp(a[0:1] - top) + b[1:2] * jnp.exp(b[0:1] - top)
        out[0:1, t0:t0 + n] = (a[2:3] + b[2:3]) - (top + jnp.log(total))

    scope = jax.named_scope

    def wait(*cps):
        for cp in cps:
            cp.wait_recv()

    with scope('proj_p'):
        project(0, 0, PIECE, rms(vx[0:PIECE].astype(F32), van[0:1, 0:D]), PIECE)
        kv_cps = share_kv(0)
    with scope('wait_x'):
        for cp in second:
            cp.wait()
        w_my0 = [load(wo.at[0], womy.at[0, pl.ds(0, QROWS)], 6), load(mn, vmn.at[:, pl.ds(0, D)], 7)]
        w_mlp0 = [load(wg.at[0], vg.at[0], 8), load(wu.at[0], vu.at[0], 9), load(wd.at[0], vd.at[0], 10)]
    with scope('proj_r'):
        project(0, PIECE, RESP, rms(vx[PIECE:ROWS].astype(F32), van[0:1, 0:D]), 0)
    w_qkv1 = load_qkv(1, 2)
    w_my1 = load(wo.at[1], womy.at[1, pl.ds(0, QROWS)], 0)
    w_head = [load(wh, vh.at[:, pl.ds(0, VOC)], 3), load(tgt, vtgt, 4), load(fn, vfn.at[pl.ds(0, D)], 5)]
    with scope('wait_kv0'):
        wait(kv_cps)
        expand(0, 0, kv[0])
    own = []
    with scope('relay0_0'):
        own.append(wo_relay_own(0, 0, wo_y0[0]))
    with scope('att0_p'):
        a_p = attend(0, C_P, my_pos, 0, PROMPT, Y_A[0])
    with scope('att0_1'):
        a_1 = attend(0, C_1, 256, 256, 384, Y_A[1])
    with scope('relay0_1'):
        own.append(wo_relay_own(0, 1, wo_y0[1]))
    with scope('att0_2'):
        a_2 = attend(0, C_2, 320, 256, 512, Y_A[2])
    with scope('relay0_2'):
        own.append(wo_relay_own(0, 2, wo_y0[2]))
    with scope('att0_3'):
        a_3 = attend(0, C_3, 448, 384, 512, Y_A[3])
    with scope('wo1'):
        wo_y1 = wo_over_y(1, (Y_WO1,))
    with scope('relay0_x0'):
        wo_relay_x(0, 0, own[0])
    with scope('own0'):
        for cp in w_my0:
            cp.wait()
        for ch in (C_A, C_2, C_3):
            merge_own(0, ch)
    with scope('turn_w'):
        w_qkv1.wait()
        for j in range(5):
            wt1[:, 128 * j:128 * (j + 1)] = wqkv[1, 128 * j:128 * (j + 1)].astype(F32).T.astype(BF16)
    with scope('relay0_x123'):
        for k in range(1, 3):
            wo_relay_x(0, k, own[k])
    with scope('wait_w0'):
        for cp in w_mlp0 + w_head:
            cp.wait()
        w_mlp1 = [load(wg.at[1], vg.at[1], 8), load(wu.at[1], vu.at[1], 9), load(wd.at[1], vd.at[1], 10)]
        for t in range(2):
            want[128 * t:128 * (t + 1)] = jnp.broadcast_to(vtgt[0:1, 128 * t:128 * (t + 1)].astype(F32), (128, 128)).T.astype(jnp.int32)
    with scope('wait_wo0'):
        wait_wo_core(0)

    with scope('wait_a0_a'):
        wait(a_p, a_1)
    with scope('merge0_a'):
        merge_attention(0, C_A, vx, (C_P, C_1))
    with scope('mlp0_a'):
        p_a = send(mlp(0, C_A, Y_P[0]))
    with scope('wait_a0_2'):
        wait(a_2)
    with scope('merge0_2'):
        merge_attention(0, C_2, vx, (C_2,))
    with scope('mlp0_2'):
        p_2 = send(mlp(0, C_2, Y_P[1]))
    with scope('wait_a0_3'):
        wait(a_3)
    with scope('merge0_3'):
        merge_attention(0, C_3, vx, (C_3,))
    with scope('mlp0_3'):
        p_3 = mlp(0, C_3, Y_P[2])
    with scope('relay1'):
        own1 = wo_relay_own(1, 0, wo_y1[0])
    with scope('wait_p0_a'):
        wait(p_a)
    with scope('close0_a'):
        x_a = close_layer0(C_A, Y_WO0[0])
        send(p_3)
    with scope('relay1_x'):
        wo_relay_x(1, 0, own1)
    with scope('wait_p0_2'):
        wait(p_2)
    with scope('close0_2'):
        x_2 = close_layer0(C_2, Y_WO0[1])
    with scope('wait_x_a'):
        wait(x_a)
    with scope('proj1_a'):
        project(1, 0, 128, rms(x1[0:128].astype(F32), van[1:2, 0:D]), PIECE)
        kv_cps = share_kv(1)
    with scope('wait_p0_3'):
        wait(p_3)
    with scope('close0_3'):
        x_3 = close_layer0(C_3, Y_WO0[2])

    with scope('wait_kv1'):
        wait(kv_cps)
        w_my1.wait()
    with scope('att1_1'):
        expand(1, 0, kv[1])
        a_1 = attend(1, C_1, 256, 256, 384, Y_A[1])
        merge_own(1, C_1)
    with scope('wait_x_2'):
        wait(x_2)
    with scope('proj1_2'):
        project(1, 128, 128, rms(x1[128:256].astype(F32), van[1:2, 0:D]), 0)
    with scope('att1_2'):
        a_2 = attend(1, C_2, 320, 256, 512, Y_A[2])
    with scope('wait_x_3'):
        wait(x_3)
    with scope('proj1_3'):
        project(1, 256, 64, rms(x1[256:320].astype(F32), van[1:2, 0:D]), 0)
    with scope('att1_3'):
        a_3 = attend(1, C_3, 448, 384, 512, Y_A[3])
        merge_own(1, C_2)
    with scope('wait_w1'):
        for cp in w_mlp1:
            cp.wait()
        wait_wo_core(1)
    with scope('wait_a1_1'):
        wait(a_1)
    with scope('merge1_1'):
        merge_attention(1, C_1, x1, (C_1,))
    with scope('mlp1_1'):
        p_1 = send(mlp(1, C_1, Y_P[0]))
    with scope('own1_3'):
        merge_own(1, C_3)
    with scope('wait_a1_2'):
        wait(a_2)
    with scope('merge1_2'):
        merge_attention(1, C_2, x1, (C_2,))
    with scope('mlp1_2'):
        p_2 = send(mlp(1, C_2, Y_P[1]))
    with scope('wait_a1_3'):
        wait(a_3)
    with scope('merge1_3'):
        merge_attention(1, C_3, x1, (C_3,))
    with scope('mlp1_3'):
        p_3 = mlp(1, C_3, Y_P[2])
    with scope('wait_p1_1'):
        wait(p_1)
    with scope('close1_1'):
        h_1 = close_layer1(C_1, Y_WO0[0])
        send(p_3)
    with scope('wait_p1_2'):
        wait(p_2)
    with scope('close1_2'):
        h_2 = close_layer1(C_2, Y_WO0[1])
    with scope('wait_h_1'):
        wait(h_1)
    with scope('head_1'):
        s_1 = head(0, C_1, Y_A[0])
    with scope('wait_p1_3'):
        wait(p_3)
    with scope('close1_3'):
        h_3 = close_layer1(C_3, Y_WO0[2])
    with scope('wait_h_2'):
        wait(h_2)
    with scope('head_2'):
        s_2 = head(1, C_2, Y_WO1)
    with scope('wait_h_3'):
        wait(h_3)
    with scope('head_3'):
        s_3 = head(2, C_3, Y_A[1])
    with scope('wait_s'):
        wait(s_1, s_2, s_3)
    with scope('finish'):
        for k, t0, n in ((0, 0, 64), (1, 64, 128), (2, 192, 64)):
            finish(k, t0, n)
    with scope('wait_sends'):
        for pool in slots.values():
            for cp in pool:
                cp.wait_send()


def solution(mesh):
    rows_spec = P(('prompts', 'resp'), None)
    in_specs = (rows_spec, P(('prompts', 'resp'), None, None), rows_spec, P(), P(),
                P(None, None, 'model', None), P(None, None, 'model', None), P(None, None, 'model', None),
                P(None, 'model', None, None), P(None, None, 'model'), P(None, None, 'model'),
                P(None, 'model', None), P(), P(None, 'model'))
    table = rope_constants()

    def local_pass(x_piece, x_own, tgt_own, attn_norm, mlp_norm, w_q, w_k, w_v, w_o, w_gate, w_up, w_down, final_norm, w_head):
        def rows_first(w):
            return jnp.transpose(w, (0, 2, 3, 1)).reshape(2, w.shape[2] * HD, D)

        any_spec = pl.BlockSpec(memory_space=pl.ANY)
        scratch = [
            pltpu.VMEM((ROWS, D), BF16), pltpu.VMEM((ROWS, 256), F32), pltpu.VMEM((1, RESP), jnp.int32),
            pltpu.VMEM((2, GAIN_PAD), F32), pltpu.VMEM((2, GAIN_PAD), F32), pltpu.VMEM((GAIN_PAD,), F32),
            pltpu.VMEM((2, 640, D), BF16), pltpu.VMEM((2, 512, D), BF16), pltpu.VMEM((2, 512, D), BF16),
            pltpu.VMEM((2, D, FF), BF16), pltpu.VMEM((2, D, FF), BF16), pltpu.VMEM((2, FF, D), BF16), pltpu.VMEM((D, VOC + 128), BF16),
            pltpu.VMEM((2, PROMPT, 128), BF16), pltpu.VMEM((2, 4, PROMPT + RESP, 128), BF16), pltpu.VMEM((D, 640), BF16), pltpu.VMEM((RESP, 128), jnp.int32),
            pltpu.VMEM((ROWS, 512), BF16), pltpu.VMEM((ROWS, 512), BF16), pltpu.VMEM((ROWS, D), F32),
            pltpu.VMEM((2, ROWS * 7 // 2, 128), BF16), pltpu.VMEM((2, ROWS * 7 // 2, 128), BF16),
            pltpu.VMEM((ROWS, D), BF16), pltpu.VMEM((128, FF), BF16),
            pltpu.VMEM((2, ROWS, D), F32), pltpu.VMEM((2, ROWS // 2, D), F32),
            pltpu.VMEM((ROWS, D), BF16), pltpu.VMEM((ROWS, D), BF16),
            pltpu.VMEM((3, 8, 128), F32), pltpu.VMEM((3, 8, 128), F32),
            pltpu.SemaphoreType.DMA((11,)), pltpu.SemaphoreType.DMA((Y_SENDS + OTHER_SENDS,)), pltpu.SemaphoreType.DMA((19,)),
        ]
        return pl.pallas_call(
            kernel,
            out_shape=jax.ShapeDtypeStruct((1, RESP), F32),
            in_specs=[any_spec] * 15,
            out_specs=pl.BlockSpec(memory_space=pltpu.VMEM),
            scratch_shapes=scratch,
            compiler_params=pltpu.CompilerParams(collective_id=0, has_side_effects=True, vmem_limit_bytes=67043328),
        )(x_piece, x_own[0], tgt_own, attn_norm, mlp_norm, rows_first(w_q), rows_first(w_k), rows_first(w_v),
          w_o.reshape(2, QROWS, D), w_gate, w_up, w_down, final_norm, w_head, jnp.asarray(table))

    return jax.shard_map(local_pass, mesh=mesh, in_specs=in_specs, out_specs=rows_spec, check_vma=False)
```

```python
import functools
import math

import jax
import jax.numpy as jnp
import numpy as np
from jax import lax
from jax.experimental import pallas as pl
from jax.experimental.pallas import tpu as pltpu
from jax.sharding import PartitionSpec as P

RMS_EPS = 1e-6
ROPE_BASE = 10000.0
NEG_BIG = -1e30
BF16 = jnp.bfloat16
F32 = jnp.float32

D = 896
HD = 64
PIECE = 64
RESP = 256
PROMPT = 256
ROWS = PIECE + RESP
FF = 2432
VOC = 2048
QROWS = 448
GROUP = 4
GAIN_PAD = 1024
C_P, C_1, C_2, C_3 = (0, 64), (64, 64), (128, 128), (256, 64)
C_A = (0, 128)
WO_QUARTER = QROWS // GROUP
WO_PIECES = (((0, 32), (32, 32), (64, 48)), ((0, 112),))
Y_WO0, Y_A, Y_WO1, Y_P, X_WO, D_WO, R_KV = (0, 1, 2), (3, 4, 5, 6), 7, (8, 9, 10), ((11, 12, 13), (14,)), (15, 16), (17, 18)
Y_SENDS, OTHER_SENDS = 8, 9
HEAD_BLOCK = 1024
FF_BLOCKS = ((0, 512), (512, 512), (1024, 512), (1536, 512), (2048, 384))


def rope_constants():
    inv = np.exp(np.arange(0, HD, 2, dtype=np.float32) * np.float32(-math.log(ROPE_BASE) / HD)).astype(np.float32)
    ang = np.arange(PROMPT + RESP, dtype=np.float32)[:, None] * inv[None, :]
    cos, sin = np.cos(ang).astype(np.float32), np.sin(ang).astype(np.float32)
    return np.concatenate([cos] * 4 + [-sin, sin] * 2, axis=1)


def mm(a, b):
    return jnp.dot(a, b, preferred_element_type=F32)


def mm_t(a, b):
    return lax.dot_general(a, b, (((1,), (1,)), ((), ())), preferred_element_type=F32)


def rms(x_f, gain):
    mean_sq = jnp.mean(x_f * x_f, axis=-1, keepdims=True)
    return (x_f * lax.rsqrt(mean_sq + RMS_EPS) * gain).astype(BF16)


def kernel(xp, xr, tgt, an, mn, wq, wk, wv, wo, wg, wu, wd, fn, wh, cs, out,
           vx, vcs, vtgt, van, vmn, vfn, wqkv, womy, woot, vg, vu, vd, vh,
           kv, kx, wt1, want, qb, amine, mo, asnd, arcv, xm, ub, part, prcv, x1, hb, st_s, st_r,
           lsem, ssem, rsem):
    me = lax.axis_index('resp')
    side = lax.axis_index('model')
    other = 1 - side
    y_peer = {'model': other}
    d_peer = {'resp': me + 1 - 2 * lax.rem(me, 2)}
    x_peer = {'resp': lax.rem(me + 2, 4)}

    barrier = pltpu.get_barrier_semaphore()
    pl.semaphore_signal(barrier, inc=1, device_id=y_peer, device_id_type=pl.DeviceIdType.MESH)
    for k in range(1, GROUP):
        pl.semaphore_signal(barrier, inc=1, device_id={'resp': lax.rem(me + k, GROUP)}, device_id_type=pl.DeviceIdType.MESH)

    def load(src, dst, k):
        cp = pltpu.make_async_copy(src, dst, lsem.at[k])
        cp.start()
        return cp

    slots = {0: [None] * Y_SENDS, 1: [None] * OTHER_SENDS}
    made = {0: 0, 1: 0}

    def remote(src, dst, peer, recv):
        pool = 0 if peer is y_peer else 1
        k = made[pool] % len(slots[pool])
        made[pool] += 1
        if slots[pool][k] is not None:
            slots[pool][k].wait_send()
        cp = pltpu.make_async_remote_copy(src_ref=src, dst_ref=dst, send_sem=ssem.at[k + pool * Y_SENDS], recv_sem=rsem.at[recv],
                                          device_id=peer, device_id_type=pl.DeviceIdType.MESH)
        slots[pool][k] = cp
        return cp

    def send(cp):
        cp.start()
        return cp

    def load_qkv(l, k):
        for src, row, n in ((wq, 0, QROWS), (wk, QROWS, HD), (wv, QROWS + HD, HD), (wv, QROWS + 2 * HD, HD)):
            load(src.at[l], wqkv.at[l, pl.ds(row, n)], k)
        return pltpu.make_async_copy(wg.at[l, pl.ds(0, 640), pl.ds(0, D)], wqkv.at[l], lsem.at[k])

    my_pos = pl.multiple_of(me * PIECE, PIECE)
    first = [load(xp, vx.at[pl.ds(0, PIECE)], 0), load(an, van.at[:, pl.ds(0, D)], 1), load_qkv(0, 2),
             load(cs.at[pl.ds(my_pos, PIECE)], vcs.at[pl.ds(0, PIECE)], 3)]
    second = [load(xr, vx.at[pl.ds(PIECE, RESP)], 4), load(cs.at[pl.ds(PROMPT, RESP)], vcs.at[pl.ds(PIECE, RESP)], 5)]

    pl.semaphore_wait(barrier, GROUP)

    def wo_slot(l, q, piece):
        start, size = WO_PIECES[l][piece]
        return pl.ds(pl.multiple_of(q * WO_QUARTER + start, 16), size)

    def wo_over_y(l, recvs):
        cps = []
        for k, recv in enumerate(recvs):
            rows = wo_slot(l, me, k)
            cps.append(send(remote(wo.at[l, rows], woot.at[l, rows], y_peer, recv)))
        return cps

    def wo_relay(l, piece, quarter, copy, to_x):
        copy.wait_recv()
        slot = woot.at[l, wo_slot(l, quarter, piece)]
        over_x = send(remote(slot, slot, x_peer, X_WO[l][piece])) if to_x else None
        send(remote(slot, slot, d_peer, D_WO[l]))
        return over_x

    def wo_relay_own(l, piece, copy):
        return wo_relay(l, piece, me, copy, True)

    def wo_relay_x(l, piece, copy):
        return wo_relay(l, piece, lax.rem(me + 2, 4), copy, False)

    def wait_wo_core(l):
        both = woot.at[l, pl.ds(0, 2 * WO_QUARTER)]
        pltpu.make_async_remote_copy(src_ref=both, dst_ref=both, send_sem=ssem.at[0], recv_sem=rsem.at[D_WO[l]],
                                     device_id=d_peer, device_id_type=pl.DeviceIdType.MESH).wait_recv()

    wo_y0 = wo_over_y(0, Y_WO0)

    zeros = jnp.zeros((512 - QROWS, D), BF16)
    for l in range(2):
        womy[l, QROWS:512] = zeros
        woot[l, QROWS:512] = zeros
    for k in range(4):
        kx[1, k, PROMPT:PROMPT + RESP] = jnp.zeros((RESP, 128), BF16)

    for cp in first:
        cp.wait()

    lane = lax.broadcasted_iota(jnp.int32, (1, 128), 1)
    lo_head = lane < HD
    lo_half = lax.rem(lane, HD) < (HD // 2)

    def expand(l, row0, pair):
        f = pair.astype(F32)
        r = pltpu.roll(f, HD, 1)
        n = pair.shape[0]
        kx[l, 0, row0:row0 + n] = jnp.where(lo_head, r, 0.0).astype(BF16)
        kx[l, 1, row0:row0 + n] = jnp.where(lo_head, 0.0, f).astype(BF16)
        kx[l, 2, row0:row0 + n] = jnp.where(lo_head, f, 0.0).astype(BF16)
        kx[l, 3, row0:row0 + n] = jnp.where(lo_head, 0.0, r).astype(BF16)

    def project(l, row0, n, hidden, piece_rows):
        y = mm(hidden, wt1[...]) if l else mm_t(hidden, wqkv[l])
        cos, sin = vcs[row0:row0 + n, 0:128], vcs[row0:row0 + n, 128:256]
        roped = []
        for j in range(4):
            b = y[:, 128 * j:128 * (j + 1)]
            partner = jnp.where(lo_half, pltpu.roll(b, 128 - HD // 2, 1), pltpu.roll(b, HD // 2, 1))
            roped.append(b * cos + partner * sin)
            qb[row0:row0 + n, 128 * j:128 * (j + 1)] = roped[-1].astype(BF16)
        pair = jnp.where(lo_head, y[:, 512:640], roped[3]).astype(BF16)
        if piece_rows:
            kv[l, pl.ds(my_pos, PIECE)] = pair[0:PIECE]
        if n > piece_rows:
            expand(l, PROMPT + row0 + piece_rows - PIECE, pair[piece_rows:n])

    def share_kv(l):
        slot = kv.at[l, pl.ds(my_pos, PIECE)]
        for k in range(1, GROUP):
            send(remote(slot, slot, {'resp': lax.rem(me + k, GROUP)}, R_KV[l]))
        three = kv.at[l, pl.ds(0, 3 * PIECE)]
        return pltpu.make_async_remote_copy(src_ref=three, dst_ref=three, send_sem=ssem.at[0], recv_sem=rsem.at[R_KV[l]],
                                            device_id=d_peer, device_id_type=pl.DeviceIdType.MESH)

    def a_base(row0):
        return row0 * 7 // 2

    def attend(l, chunk, base, vis, nk, recv):
        row0, n = chunk
        k_even, k_odd, v_even, v_odd = (kx[l, k, 0:nk] for k in range(4))
        q = [qb[row0:row0 + n, 128 * j:128 * (j + 1)] for j in range(4)]
        s_even = mm_t(jnp.concatenate(q, axis=0), k_even)
        s_odd = mm_t(jnp.concatenate(q[:3], axis=0), k_odd)
        keep = (lax.broadcasted_iota(jnp.int32, (n, nk - vis), 1) + vis) <= (base + lax.broadcasted_iota(jnp.int32, (n, nk - vis), 0))

        def probs(s):
            tail = jnp.where(keep, s[:, vis:], NEG_BIG)
            s = jnp.concatenate([s[:, :vis], tail], axis=1) if vis else tail
            top = jnp.max(s, axis=-1, keepdims=True)
            e = jnp.exp2((s - top) * (math.log2(math.e) / math.sqrt(HD)))
            return (e * (1.0 / jnp.sum(e, axis=-1, keepdims=True))).astype(BF16)

        p_even = jnp.concatenate([probs(s_even[j * n:(j + 1) * n]) for j in range(4)], axis=0)
        p_odd = jnp.concatenate([probs(s_odd[j * n:(j + 1) * n]) for j in range(3)], axis=0)
        o_even = mm(p_even, v_even)
        o_odd = mm(p_odd, v_odd)
        ab = a_base(row0)
        for j in range(3):
            blk = (o_even[j * n:(j + 1) * n] + o_odd[j * n:(j + 1) * n]).astype(BF16)
            amine[row0:row0 + n, 128 * j:128 * (j + 1)] = blk
            asnd[l, ab + j * n:ab + (j + 1) * n] = blk
        last = o_even[3 * n:4 * n]
        amine[row0:row0 + n, 384:512] = last.astype(BF16)
        asnd[l, ab + 3 * n:ab + 7 * n // 2] = (last[:n // 2] + pltpu.roll(last[n // 2:], HD, 1)).astype(BF16)
        rows = pl.ds(ab, 7 * n // 2)
        return send(remote(asnd.at[l, rows], arcv.at[l, rows], y_peer, recv))

    def merge_own(l, chunk):
        row0, n = chunk
        mo[row0:row0 + n] = mm(amine[row0:row0 + n], womy[l])

    def received(l, chunk):
        row0, n = chunk
        ab = a_base(row0)
        packed = arcv[l, ab + 3 * n:ab + 7 * n // 2].astype(F32)
        last = jnp.concatenate([packed, pltpu.roll(packed, HD, 1)], axis=0).astype(BF16)
        return jnp.concatenate([arcv[l, ab + j * n:ab + (j + 1) * n] for j in range(3)] + [last], axis=1)

    def merge_attention(l, chunk, x_ref, parts):
        row0, n = chunk
        a_oth = jnp.concatenate([received(l, p) for p in parts], axis=0)
        proj = mo[row0:row0 + n] + mm(a_oth, woot[l])
        xm[row0:row0 + n] = (x_ref[row0:row0 + n].astype(F32) + proj).astype(BF16)

    def mlp(l, chunk, recv):
        row0, n = chunk
        g = rms(xm[row0:row0 + n].astype(F32), vmn[l:l + 1, 0:D])
        for b0, bn in FF_BLOCKS:
            gate = mm(g, vg[l, :, b0:b0 + bn])
            up = mm(g, vu[l, :, b0:b0 + bn])
            ub[0:n, b0:b0 + bn] = (gate * (1.0 / (1.0 + jnp.exp(-gate))) * up).astype(BF16)
        part[l, row0:row0 + n] = mm(ub[0:n], vd[l])
        h = n // 2
        away = pl.ds(pl.multiple_of(row0 + other * h, 16), h)
        return remote(part.at[l, away], prcv.at[l, pl.ds(row0 // 2, h)], y_peer, recv)

    def home_rows(chunk):
        row0, n = chunk
        return pl.ds(pl.multiple_of(row0 + side * (n // 2), 16), n // 2)

    def home_sum(l, chunk):
        row0, n = chunk
        rows = home_rows(chunk)
        total = part[l, rows] + prcv[l, row0 // 2:row0 // 2 + n // 2]
        return (xm[rows].astype(F32) + total).astype(BF16)

    def close_layer0(chunk, recv):
        rows = home_rows(chunk)
        x1[rows] = home_sum(0, chunk)
        return send(remote(x1.at[rows], x1.at[rows], y_peer, recv))

    def close_layer1(chunk, recv):
        rows = home_rows(chunk)
        hb[rows] = rms(home_sum(1, chunk).astype(F32), vfn[...].reshape(1, GAIN_PAD)[:, 0:D])
        return send(remote(hb.at[rows], hb.at[rows], y_peer, recv))

    def head(k, chunk, recv):
        row0, n = chunk
        hidden = hb[row0:row0 + n]
        ids0 = side * VOC + lax.broadcasted_iota(jnp.int32, (1, HEAD_BLOCK), 1)
        wanted = want[row0 - PIECE:row0 - PIECE + n, 0:1]
        tops, sums, picked = [], [], None
        for b in range(VOC // HEAD_BLOCK):
            lg = mm(hidden, vh[:, HEAD_BLOCK * b:HEAD_BLOCK * (b + 1)])
            tops.append(jnp.max(lg, axis=-1, keepdims=True))
            sums.append(jnp.sum(jnp.exp(lg - tops[-1]), axis=-1, keepdims=True))
            hit = jnp.sum(jnp.where(ids0 + HEAD_BLOCK * b == wanted, lg, 0.0), axis=-1, keepdims=True)
            picked = hit if picked is None else picked + hit
        top = functools.reduce(jnp.maximum, tops)
        total = sum(t * jnp.exp(m - top) for t, m in zip(sums, tops))
        table = jnp.where(lane == 0, top, jnp.where(lane == 1, total, picked))
        st_s[k, :, 0:n] = table.T[0:8]
        return send(remote(st_s.at[k], st_r.at[k], y_peer, recv))

    def finish(k, t0, n):
        a, b = st_s[k, :, 0:n], st_r[k, :, 0:n]
        top = jnp.maximum(a[0:1], b[0:1])
        total = a[1:2] * jnp.exp(a[0:1] - top) + b[1:2] * jnp.exp(b[0:1] - top)
        out[:, t0:t0 + n] = jnp.broadcast_to((a[2:3] + b[2:3]) - (top + jnp.log(total)), (8, n))

    scope = jax.named_scope

    def wait(*cps):
        for cp in cps:
            cp.wait_recv()

    with scope('proj_p'):
        project(0, 0, PIECE, rms(vx[0:PIECE].astype(F32), van[0:1, 0:D]), PIECE)
        kv_cps = share_kv(0)
    with scope('wait_x'):
        for cp in second:
            cp.wait()
        w_my0 = [load(wo.at[0], womy.at[0, pl.ds(0, QROWS)], 6), load(mn, vmn.at[:, pl.ds(0, D)], 7)]
        w_mlp0 = [load(wg.at[0], vg.at[0], 8), load(wu.at[0], vu.at[0], 9), load(wd.at[0], vd.at[0], 10)]
    with scope('proj_r'):
        project(0, PIECE, RESP, rms(vx[PIECE:ROWS].astype(F32), van[0:1, 0:D]), 0)
    w_qkv1 = load_qkv(1, 2)
    w_my1 = load(wo.at[1], womy.at[1, pl.ds(0, QROWS)], 0)
    w_head = [load(wh, vh.at[:, pl.ds(0, VOC)], 3), load(tgt, vtgt, 4), load(fn, vfn.at[pl.ds(0, D)], 5)]
    with scope('wait_kv0'):
        wait(kv_cps)
        expand(0, 0, kv[0])
    own = []
    with scope('relay0_0'):
        own.append(wo_relay_own(0, 0, wo_y0[0]))
    with scope('att0_p'):
        a_p = attend(0, C_P, my_pos, 0, PROMPT, Y_A[0])
    with scope('att0_1'):
        a_1 = attend(0, C_1, 256, 256, 384, Y_A[1])
    with scope('relay0_1'):
        own.append(wo_relay_own(0, 1, wo_y0[1]))
    with scope('att0_2'):
        a_2 = attend(0, C_2, 320, 256, 512, Y_A[2])
    with scope('relay0_2'):
        own.append(wo_relay_own(0, 2, wo_y0[2]))
    with scope('att0_3'):
        a_3 = attend(0, C_3, 448, 384, 512, Y_A[3])
    with scope('wo1'):
        wo_y1 = wo_over_y(1, (Y_WO1,))
    with scope('relay0_x0'):
        wo_relay_x(0, 0, own[0])
    with scope('own0'):
        for cp in w_my0:
            cp.wait()
        for ch in (C_A, C_2, C_3):
            merge_own(0, ch)
    with scope('turn_w'):
        w_qkv1.wait()
        for j in range(5):
            wt1[:, 128 * j:128 * (j + 1)] = wqkv[1, 128 * j:128 * (j + 1)].astype(F32).T.astype(BF16)
    with scope('relay0_x123'):
        for k in range(1, 3):
            wo_relay_x(0, k, own[k])
    with scope('wait_w0'):
        for cp in w_mlp0 + w_head:
            cp.wait()
        w_mlp1 = [load(wg.at[1], vg.at[1], 8), load(wu.at[1], vu.at[1], 9), load(wd.at[1], vd.at[1], 10)]
        for t in range(2):
            want[128 * t:128 * (t + 1)] = jnp.broadcast_to(vtgt[0:1, 128 * t:128 * (t + 1)].astype(F32), (128, 128)).T.astype(jnp.int32)
    with scope('wait_wo0'):
        wait_wo_core(0)

    with scope('wait_a0_a'):
        wait(a_p, a_1)
    with scope('merge0_a'):
        merge_attention(0, C_A, vx, (C_P, C_1))
    with scope('mlp0_a'):
        p_a = send(mlp(0, C_A, Y_P[0]))
    with scope('wait_a0_2'):
        wait(a_2)
    with scope('merge0_2'):
        merge_attention(0, C_2, vx, (C_2,))
    with scope('mlp0_2'):
        p_2 = send(mlp(0, C_2, Y_P[1]))
    with scope('wait_a0_3'):
        wait(a_3)
    with scope('merge0_3'):
        merge_attention(0, C_3, vx, (C_3,))
    with scope('mlp0_3'):
        p_3 = mlp(0, C_3, Y_P[2])
    with scope('relay1'):
        own1 = wo_relay_own(1, 0, wo_y1[0])
    with scope('wait_p0_a'):
        wait(p_a)
    with scope('close0_a'):
        x_a = close_layer0(C_A, Y_WO0[0])
        send(p_3)
    with scope('relay1_x'):
        wo_relay_x(1, 0, own1)
    with scope('wait_p0_2'):
        wait(p_2)
    with scope('close0_2'):
        x_2 = close_layer0(C_2, Y_WO0[1])
    with scope('wait_x_a'):
        wait(x_a)
    with scope('proj1_a'):
        project(1, 0, 128, rms(x1[0:128].astype(F32), van[1:2, 0:D]), PIECE)
        kv_cps = share_kv(1)
    with scope('wait_p0_3'):
        wait(p_3)
    with scope('close0_3'):
        x_3 = close_layer0(C_3, Y_WO0[2])

    with scope('wait_kv1'):
        wait(kv_cps)
        w_my1.wait()
    with scope('att1_1'):
        expand(1, 0, kv[1])
        a_1 = attend(1, C_1, 256, 256, 384, Y_A[1])
        merge_own(1, C_1)
    with scope('wait_x_2'):
        wait(x_2)
    with scope('proj1_2'):
        project(1, 128, 128, rms(x1[128:256].astype(F32), van[1:2, 0:D]), 0)
    with scope('att1_2'):
        a_2 = attend(1, C_2, 320, 256, 512, Y_A[2])
    with scope('wait_x_3'):
        wait(x_3)
    with scope('proj1_3'):
        project(1, 256, 64, rms(x1[256:320].astype(F32), van[1:2, 0:D]), 0)
    with scope('att1_3'):
        a_3 = attend(1, C_3, 448, 384, 512, Y_A[3])
        merge_own(1, C_2)
    with scope('wait_w1'):
        for cp in w_mlp1:
            cp.wait()
        wait_wo_core(1)
    with scope('wait_a1_1'):
        wait(a_1)
    with scope('merge1_1'):
        merge_attention(1, C_1, x1, (C_1,))
    with scope('mlp1_1'):
        p_1 = send(mlp(1, C_1, Y_P[0]))
    with scope('own1_3'):
        merge_own(1, C_3)
    with scope('wait_a1_2'):
        wait(a_2)
    with scope('merge1_2'):
        merge_attention(1, C_2, x1, (C_2,))
    with scope('mlp1_2'):
        p_2 = send(mlp(1, C_2, Y_P[1]))
    with scope('wait_a1_3'):
        wait(a_3)
    with scope('merge1_3'):
        merge_attention(1, C_3, x1, (C_3,))
    with scope('mlp1_3'):
        p_3 = mlp(1, C_3, Y_P[2])
    with scope('wait_p1_1'):
        wait(p_1)
    with scope('close1_1'):
        h_1 = close_layer1(C_1, Y_WO0[0])
        send(p_3)
    with scope('wait_p1_2'):
        wait(p_2)
    with scope('close1_2'):
        h_2 = close_layer1(C_2, Y_WO0[1])
    with scope('wait_h_1'):
        wait(h_1)
    with scope('head_1'):
        s_1 = head(0, C_1, Y_A[0])
    with scope('wait_p1_3'):
        wait(p_3)
    with scope('close1_3'):
        h_3 = close_layer1(C_3, Y_WO0[2])
    with scope('wait_h_2'):
        wait(h_2)
    with scope('head_2'):
        s_2 = head(1, C_2, Y_WO1)
    with scope('wait_h_3'):
        wait(h_3)
    with scope('head_3'):
        s_3 = head(2, C_3, Y_A[1])
    with scope('wait_s'):
        wait(s_1, s_2, s_3)
    with scope('finish'):
        for k, t0, n in ((0, 0, 64), (1, 64, 128), (2, 192, 64)):
            finish(k, t0, n)
    with scope('wait_sends'):
        for pool in slots.values():
            for cp in pool:
                cp.wait_send()


def solution(mesh):
    rows_spec = P(('prompts', 'resp'), None)
    in_specs = (rows_spec, P(('prompts', 'resp'), None, None), rows_spec, P(), P(),
                P(None, None, 'model', None), P(None, None, 'model', None), P(None, None, 'model', None),
                P(None, 'model', None, None), P(None, None, 'model'), P(None, None, 'model'),
                P(None, 'model', None), P(), P(None, 'model'))
    table = rope_constants()

    def local_pass(x_piece, x_own, tgt_own, attn_norm, mlp_norm, w_q, w_k, w_v, w_o, w_gate, w_up, w_down, final_norm, w_head):
        def rows_first(w):
            return jnp.transpose(w, (0, 2, 3, 1)).reshape(2, w.shape[2] * HD, D)

        any_spec = pl.BlockSpec(memory_space=pl.ANY)
        scratch = [
            pltpu.VMEM((ROWS, D), BF16), pltpu.VMEM((ROWS, 256), F32), pltpu.VMEM((1, RESP), jnp.int32),
            pltpu.VMEM((2, GAIN_PAD), F32), pltpu.VMEM((2, GAIN_PAD), F32), pltpu.VMEM((GAIN_PAD,), F32),
            pltpu.VMEM((2, 640, D), BF16), pltpu.VMEM((2, 512, D), BF16), pltpu.VMEM((2, 512, D), BF16),
            pltpu.VMEM((2, D, FF), BF16), pltpu.VMEM((2, D, FF), BF16), pltpu.VMEM((2, FF, D), BF16), pltpu.VMEM((D, VOC + 128), BF16),
            pltpu.VMEM((2, PROMPT, 128), BF16), pltpu.VMEM((2, 4, PROMPT + RESP, 128), BF16), pltpu.VMEM((D, 640), BF16), pltpu.VMEM((RESP, 128), jnp.int32),
            pltpu.VMEM((ROWS, 512), BF16), pltpu.VMEM((ROWS, 512), BF16), pltpu.VMEM((ROWS, D), F32),
            pltpu.VMEM((2, ROWS * 7 // 2, 128), BF16), pltpu.VMEM((2, ROWS * 7 // 2, 128), BF16),
            pltpu.VMEM((ROWS, D), BF16), pltpu.VMEM((128, FF), BF16),
            pltpu.VMEM((2, ROWS, D), F32), pltpu.VMEM((2, ROWS // 2, D), F32),
            pltpu.VMEM((ROWS, D), BF16), pltpu.VMEM((ROWS, D), BF16),
            pltpu.VMEM((3, 8, 128), F32), pltpu.VMEM((3, 8, 128), F32),
            pltpu.SemaphoreType.DMA((11,)), pltpu.SemaphoreType.DMA((Y_SENDS + OTHER_SENDS,)), pltpu.SemaphoreType.DMA((19,)),
        ]
        rows = pl.pallas_call(
            kernel,
            out_shape=jax.ShapeDtypeStruct((8, RESP), F32),
            in_specs=[any_spec] * 15,
            out_specs=pl.BlockSpec(memory_space=pltpu.VMEM),
            scratch_shapes=scratch,
            compiler_params=pltpu.CompilerParams(collective_id=0, has_side_effects=True, vmem_limit_bytes=56524800),
        )(x_piece, x_own[0], tgt_own, attn_norm, mlp_norm, rows_first(w_q), rows_first(w_k), rows_first(w_v),
          w_o.reshape(2, QROWS, D), w_gate, w_up, w_down, final_norm, w_head, jnp.asarray(table))
        return rows[0:1]

    return jax.shard_map(local_pass, mesh=mesh, in_specs=in_specs, out_specs=rows_spec, check_vma=False)
```
